512 devices in a mesh: grp: 2 (over core), row: 16 (over x, y_hi), col: 16 (over y_lo, z).
Axes of the slice: x: 4, y: 8 (y_hi: 4, y_lo: 2; y = y_hi * 2 + y_lo), z: 8, core: 2. Of those that a mesh axis runs over, the one named last changes fastest.
Arguments:
- front: float32 [16384, 16384], P(('grp', 'row'), 'col'), may hold values from -9 to 1400, as said below
- prev_lower: bfloat16 [16384, 256], P(('grp', 'row', 'col')), may hold values from -0.035888672 to 0.035888672
- prev_pivots: float32 [256], replicated, may hold values from 150 to 400
- pivot_order: int32 [2, 256], replicated, may hold values from 0 to 255, each once within a row
Outputs:
- schur: float32 [16384, 16384], P(('grp', 'row'), 'col')
- panels_scaled: float32 [16384, 512], P(('grp', 'row', 'col'))
- pivots: float32 [512], replicated
The draws below stay inside these ranges and needn't reach their ends.
Inputs may be any that keep to these rules, and one draw needn't show every extreme that they name: front is symmetric and positive definite, and stays so after the update by the pending panel, so that every Schur complement of the window is positive definite. Each row of pivot_order names every number of 0 to 255 once.
All inputs are finite; a program needn't handle non-finite values.
Results may differ from the reference program's by a relative error of at most 0.0003.
Values may be sent and summed in bfloat16 or wider, within the bound.
A program may use at most 128 MiB of HBM per device.

```python
import math
import jax
import jax.numpy as jnp
from jax import lax

R = 16384
PB = 256
STEPS = 2


def draw_front(key, part):
    leading, second = jax.random.split(key, 2)
    entries = jnp.clip(jax.random.normal(leading, (R, R), jnp.float32), -6.0, 6.0)
    symmetric = (entries + entries.T) * 0.70710678
    diag_values = jax.random.uniform(second, (R,), jnp.float32, 400.0, 700.0)
    positions = jnp.arange(R, dtype=jnp.int32)
    symmetric = symmetric.at[positions, positions].set(diag_values)
    return symmetric


def steps_of(rng, extent, pieces, least, high):
    loudness, own = 1.0, jax.random.fold_in(rng, 6)
    for position, parts in pieces:
        heights = jnp.exp(jax.random.uniform(jax.random.fold_in(own, position), (parts,), jnp.float32, least / len(pieces), high / len(pieces)))
        loudness = loudness * jnp.repeat(heights, extent[position] // parts).reshape([-1 if axis == position else 1 for axis in range(len(extent))])
    return loudness


def bell_draw(rng, shape, deviation, bound, pieces=(), kind=jnp.bfloat16):
    array = deviation * jax.random.normal(rng, shape, jnp.float32)
    if pieces:
        array = array * steps_of(rng, shape, pieces, -0.22, 0.18)
    return jnp.clip(array, -bound, bound).astype(kind)


def setup_inputs(seed: int = 0) -> dict:
    key_list = jax.random.split(jax.random.key(seed), 5)
    return {
        "front": draw_front(jax.random.fold_in(key_list[4], 71), 0),
        "prev_lower": bell_draw(key_list[1], (R, PB), (0.096 * PB ** -0.5), 0.035888672, ((0, 512),)),
        "prev_pivots": jnp.clip(jnp.exp(jax.random.uniform(key_list[2], (PB,), jnp.float32, math.log(150.0), math.log(400.0))), 150.0, 400.0),
        "pivot_order": jax.vmap(lambda own: jax.random.permutation(own, PB))(jax.random.split(key_list[3], STEPS)).reshape((STEPS, PB)).astype(jnp.int32),
    }


def apply_panel(matrix, factor_rows, pivot_values):
    exact = lax.Precision.HIGHEST
    scaled = (factor_rows.astype(jnp.float32) * pivot_values).astype(jnp.bfloat16)
    return matrix - jnp.dot(scaled.astype(jnp.float32), factor_rows.astype(jnp.float32).T, precision=exact)

def reference(front, prev_lower, prev_pivots, pivot_order):
    exact = lax.Precision.HIGHEST
    panel_width = prev_lower.shape[1]
    panel_count = pivot_order.shape[0]
    row_ids = jnp.arange(front.shape[0], dtype=jnp.int32)
    matrix = front
    factor_rows = prev_lower
    pivot_values = prev_pivots
    outputs = []
    pivot_list = []
    for panel_index in range(panel_count):
        matrix = apply_panel(matrix, factor_rows, pivot_values)
        start = panel_index * panel_width
        panel_cols = matrix[:, start:start + panel_width]
        select = (pivot_order[panel_index][:, None] == jnp.arange(panel_width, dtype=jnp.int32)[None, :]).astype(jnp.float32)
        diagonal_block = panel_cols[start:start + panel_width]
        permuted = jnp.dot(jnp.dot(select, diagonal_block, precision=exact), select.T, precision=exact)
        cholesky_factor = jnp.linalg.cholesky(permuted)
        root_diag = jnp.diagonal(cholesky_factor)
        moved = jnp.dot(panel_cols, select.T, precision=exact)
        solved = lax.linalg.triangular_solve(cholesky_factor, moved, left_side=False, lower=True, transpose_a=True)
        live_rows = (row_ids >= start)[:, None]
        shown_rows = jnp.where(live_rows, solved / root_diag, jnp.zeros_like(solved)).astype(jnp.bfloat16)
        pivot_values = root_diag * root_diag
        outputs.append(shown_rows.astype(jnp.float32) * pivot_values)
        pivot_list.append(pivot_values)
        trailing_rows = (row_ids >= start + panel_width)[:, None]
        factor_rows = jnp.where(trailing_rows, shown_rows, jnp.zeros_like(shown_rows))
    return (matrix, jnp.concatenate(outputs, axis=1), jnp.concatenate(pivot_list))
```

```python
import jax
import jax.numpy as jnp
from jax import lax
from jax.experimental import pallas as pl
from jax.experimental.pallas import tpu as pltpu
from jax.sharding import PartitionSpec as P

F32 = jnp.float32
BF16 = jnp.bfloat16
EXACT = lax.Precision.HIGHEST
MESH = pl.DeviceIdType.MESH
CHUNK = 32
WIDTH = 256
HALF = 128
VMEM_LIMIT = 60 * 1024 * 1024


def place():
    return lax.axis_index("grp"), lax.axis_index("row"), lax.axis_index("col")


def remote(src, dst, send_sem, recv_sem, device):
    return pltpu.make_async_remote_copy(
        src_ref=src, dst_ref=dst, send_sem=send_sem, recv_sem=recv_sem,
        device_id=device, device_id_type=MESH,
    )


def signal(barrier, device):
    pl.semaphore_signal(barrier, inc=1, device_id=device, device_id_type=MESH)


def turn(value, step, size):
    return lax.rem(value + step + size, size)


def block(ref, number, rows):
    return ref.at[pl.ds(pl.multiple_of(number * rows, rows), rows)]


class Spread:
    def __init__(self, chunk, rows, cols, sems):
        self.chunk, self.rows, self.cols = chunk, rows, cols
        (self.zs, self.zr, self.fs, self.fr, self.ps, self.pr,
         self.xs, self.xr, self.cs, self.cr, self.own) = sems
        g, r, c = place()
        self.g, self.r, self.c = g, r, c
        self.x, self.yh, self.yl, self.z = r // 4, r % 4, c // 8, c % 8

    @staticmethod
    def semaphores():
        dma = pltpu.SemaphoreType.DMA
        return [dma((7,)), dma((7,)), dma((8,)), dma((8,)), dma((4,)), dma((4,)),
                dma((3,)), dma((3,)), dma((4,)), dma((4,)), dma((2,))]

    def target(self, j):
        return (self.r % 2, (self.c // 4) * 4 + j, self.g * 8 + self.r // 2)

    def source(self, i):
        return (self.c // 8, (2 * self.c + self.g) % 16, self.x * 4 + i)

    def is_me(self, device):
        return (device[0] == self.g) & (device[1] == self.r) & (device[2] == self.c)

    def greet(self, barrier):
        g, r, c = self.g, self.r, self.c
        for dz in range(1, 8):
            signal(barrier, (g, r, self.yl * 8 + turn(self.z, -dz, 8)))
        signal(barrier, (g, r, (1 - self.yl) * 8 + self.z))
        for dx in range(1, 4):
            signal(barrier, (g, turn(self.x, -dx, 4) * 4 + self.yh, c))
        signal(barrier, (1 - g, r, c))
        count = jnp.int32(12)
        for i in range(4):
            source = self.source(i)

            @pl.when(jnp.logical_not(self.is_me(source)))
            def _():
                signal(barrier, source)

            count += jnp.where(self.is_me(self.target(i)), 0, 1)
        return count

    def crossing(self, j):
        slot = (self.r % 2) * 16 + self.c
        return remote(self.chunk, block(self.cols, slot, CHUNK), self.ps.at[j],
                      self.pr.at[self.c % 4], self.target(j))

    def arriving(self, i):
        slot = self.g * 16 + self.x * 4 + i
        return remote(self.chunk, block(self.cols, slot, CHUNK), self.ps.at[i],
                      self.pr.at[i], self.source(i))

    def crossing_own(self):
        slot = (self.r % 2) * 16 + self.c
        return pltpu.make_async_copy(self.chunk, block(self.cols, slot, CHUNK), self.own.at[0])

    def across_z(self, dz, slot_z):
        return remote(self.chunk, block(self.rows, self.yl * 8 + slot_z, CHUNK),
                      self.zs.at[dz - 1], self.zr.at[dz - 1],
                      (self.g, self.r, self.yl * 8 + turn(self.z, dz, 8)))

    def partner(self, dz, side):
        slot = side * 8 + turn(self.z, -dz, 8)
        src = self.chunk if dz == 0 else block(self.rows, slot, CHUNK)
        return remote(src, block(self.rows, slot, CHUNK), self.fs.at[dz], self.fr.at[dz],
                      (self.g, self.r, (1 - self.yl) * 8 + self.z))

    def across_x(self, dx, x):
        part = block(self.cols, self.g * 4 + x, 4 * CHUNK)
        return remote(part, part, self.xs.at[dx - 1], self.xr.at[dx - 1],
                      (self.g, turn(self.x, dx, 4) * 4 + self.yh, self.c))

    def sibling(self, dx, grp):
        part = block(self.cols, grp * 4 + turn(self.x, -dx, 4), 4 * CHUNK)
        return remote(part, part, self.cs.at[dx], self.cr.at[dx], (1 - self.g, self.r, self.c))

    def own_row_copy(self):
        return pltpu.make_async_copy(self.chunk, block(self.rows, self.c, CHUNK), self.own.at[1])

    def begin(self):
        for j in range(4):
            me = self.is_me(self.target(j))

            @pl.when(me)
            def _():
                self.crossing_own().start()

            @pl.when(jnp.logical_not(me))
            def _():
                self.crossing(j).start()

        for dz in range(1, 8):
            self.across_z(dz, self.z).start()
        self.partner(0, self.yl).start()
        self.own_row_copy().start()

    def first_columns(self):
        for i in range(4):
            me = self.is_me(self.source(i))

            @pl.when(me)
            def _():
                self.crossing_own().wait()

            @pl.when(jnp.logical_not(me))
            def _():
                self.arriving(i).wait_recv()

        for dx in range(1, 4):
            self.across_x(dx, self.x).start()
        self.sibling(0, self.g).start()

    def pass_rows(self):
        for dz in range(1, 8):
            self.across_z(dz, turn(self.z, -dz, 8)).wait_recv()
            self.partner(dz, self.yl).start()

    def pass_columns(self):
        for dx in range(1, 4):
            self.across_x(dx, turn(self.x, -dx, 4)).wait_recv()
            self.sibling(dx, self.g).start()

    def finish(self):
        self.own_row_copy().wait()
        for dz in range(8):
            self.partner(dz, 1 - self.yl).wait_recv()
        for dx in range(4):
            self.sibling(dx, 1 - self.g).wait_recv()

    def drain(self):
        for j in range(4):
            @pl.when(jnp.logical_not(self.is_me(self.target(j))))
            def _():
                self.crossing(j).wait_send()

        for dz in range(1, 8):
            self.across_z(dz, self.z).wait_send()
        for dz in range(8):
            self.partner(dz, self.yl).wait_send()
        for dx in range(1, 4):
            self.across_x(dx, self.x).wait_send()
        for dx in range(4):
            self.sibling(dx, self.g).wait_send()


class Corner:
    def __init__(self, front, corner, sems):
        self.front, self.corner = front, corner
        self.ts, self.tr, self.ys, self.yr, self.xs, self.xr, self.cs, self.cr = sems
        self.g, self.r, self.c = place()
        self.x, self.yh = self.r // 4, self.r % 4
        self.q = self.g * 16 + self.r
        self.rows = corner.shape[0] // 32
        self.lanes = corner.shape[1]

    @staticmethod
    def semaphores():
        dma = pltpu.SemaphoreType.DMA
        return [dma((32,)), dma, dma((3,)), dma((3,)), dma((3,)), dma((3,)), dma((4,)), dma((4,))]

    def greet(self, barrier):
        @pl.when(self.c == 0)
        def _():
            for dy in range(1, 4):
                signal(barrier, (self.g, self.x * 4 + turn(self.yh, -dy, 4), self.c))

            @pl.when(self.q != 0)
            def _():
                signal(barrier, (0, 0, 0))

        return jnp.where(self.c == 0, 3, 0) + jnp.where((self.q == 0) & (self.c == 0), 31, 0)

    def piece(self, slot):
        start = pl.multiple_of(slot * self.rows, self.rows)
        return self.front.at[pl.ds(start, self.rows), pl.ds(0, self.lanes)]

    def handing(self, slot):
        return remote(self.piece(slot), block(self.corner, slot, self.rows), self.ts.at[slot],
                      self.tr, (slot // 16, slot % 16, 0))

    def keeping(self):
        return pltpu.make_async_copy(self.piece(0), block(self.corner, 0, self.rows), self.tr)

    def across_y(self, dy, yh):
        part = block(self.corner, self.g * 16 + self.x * 4 + yh, self.rows)
        return remote(part, part, self.ys.at[dy - 1], self.yr.at[dy - 1],
                      (self.g, self.x * 4 + turn(self.yh, dy, 4), self.c))

    def across_x(self, dx, x):
        part = block(self.corner, self.g * 4 + x, 4 * self.rows)
        return remote(part, part, self.xs.at[dx - 1], self.xr.at[dx - 1],
                      (self.g, turn(self.x, dx, 4) * 4 + self.yh, self.c))

    def sibling(self, dx, grp):
        part = block(self.corner, grp * 4 + turn(self.x, -dx, 4), 4 * self.rows)
        return remote(part, part, self.cs.at[dx], self.cr.at[dx], (1 - self.g, self.r, self.c))

    def begin(self):
        @pl.when((self.q == 0) & (self.c == 0))
        def _():
            self.keeping().start()

            @pl.loop(1, 32)
            def _(slot):
                self.handing(slot).start()

    def relay(self):
        @pl.when(self.c == 0)
        def _():
            @pl.when(self.q == 0)
            def _():
                self.keeping().wait()

            @pl.when(self.q != 0)
            def _():
                self.handing(self.q).wait_recv()

            for dy in range(1, 4):
                self.across_y(dy, self.yh).start()
            for dy in range(1, 4):
                self.across_y(dy, turn(self.yh, -dy, 4)).wait_recv()
            for dx in range(1, 4):
                self.across_x(dx, self.x).start()
            self.sibling(0, self.g).start()
            for dx in range(1, 4):
                self.across_x(dx, turn(self.x, -dx, 4)).wait_recv()
                self.sibling(dx, self.g).start()
            for dx in range(4):
                self.sibling(dx, 1 - self.g).wait_recv()

    def drain(self):
        @pl.when(self.c == 0)
        def _():
            @pl.when(self.q == 0)
            def _():
                @pl.loop(1, 32)
                def _(slot):
                    self.handing(slot).wait_send()

            for dy in range(1, 4):
                self.across_y(dy, self.yh).wait_send()
            for dx in range(1, 4):
                self.across_x(dx, self.x).wait_send()
            for dx in range(4):
                self.sibling(dx, self.g).wait_send()


def gather_kernel(chunk, front, rows, cols, corner, *sems):
    split = len(Spread.semaphores())
    spread = Spread(chunk, rows, cols, sems[:split])
    square = Corner(front, corner, sems[split:])
    barrier = pltpu.get_barrier_semaphore()
    count = spread.greet(barrier) + square.greet(barrier)
    pl.semaphore_wait(barrier, count)
    square.begin()
    spread.begin()
    spread.first_columns()
    spread.pass_rows()
    spread.pass_columns()
    square.relay()
    spread.finish()
    spread.drain()
    square.drain()


def share_kernel(left, right, pivots, chunk, second, shared, rows, cols, *sems):
    split = len(Spread.semaphores())
    spread = Spread(chunk, rows, cols, sems[:split])
    send, recv, own = sems[split:]
    g, r, c = place()
    barrier = pltpu.get_barrier_semaphore()
    count = spread.greet(barrier)

    @pl.when(c != 0)
    def _():
        signal(barrier, (g, r, 0))

    pl.semaphore_wait(barrier, count + jnp.where(c == 0, 15, 0))

    def handed(number, to):
        device = (g, r, to)
        if number == 0:
            return remote(block(left, to, CHUNK), chunk, send.at[0, to], recv.at[0], device)
        if number == 1:
            return remote(block(right, to, CHUNK), second, send.at[1, to], recv.at[1], device)
        return remote(pivots, shared, send.at[2, to], recv.at[2], device)

    kept = (
        pltpu.make_async_copy(block(left, 0, CHUNK), chunk, own.at[0]),
        pltpu.make_async_copy(block(right, 0, CHUNK), second, own.at[1]),
        pltpu.make_async_copy(pivots, shared, own.at[2]),
    )

    @pl.when(c == 0)
    def _():
        for number in range(3):
            for to in range(1, 16):
                handed(number, to).start()
            kept[number].start()
        kept[0].wait()

    @pl.when(c != 0)
    def _():
        handed(0, c).wait_recv()

    spread.begin()
    spread.first_columns()
    spread.pass_rows()
    spread.pass_columns()
    spread.finish()
    spread.drain()

    @pl.when(c == 0)
    def _():
        for number in range(3):
            for to in range(1, 16):
                handed(number, to).wait_send()
        kept[1].wait()
        kept[2].wait()

    @pl.when(c != 0)
    def _():
        handed(1, c).wait_recv()
        handed(2, c).wait_recv()


def times(a, b, dims, precision=None):
    return lax.dot_general(
        a, b, (dims, ((), ())), precision=precision, preferred_element_type=F32
    )


NN = ((1,), (0,))
NT = ((1,), (1,))
TN = ((0,), (0,))


def eliminate(work, inverse, pivots, recips, columns, small):
    def panel(first):
        def step(number, carry):
            top = pl.multiple_of(number * 8, 8)
            lane = [jnp.full((8, HALF), top + k, jnp.int32) for k in range(8)]
            head = work[pl.ds(top, 8), 0:HALF]
            for k in range(8):
                small[8 * k:8 * k + 8, :] = jnp.take_along_axis(head, lane[k], axis=1)
            for i in range(first, 16):
                tile = work[8 * i:8 * i + 8, 0:HALF]
                for k in range(8):
                    columns[8 * (8 * i + k):8 * (8 * i + k) + 8, :] = jnp.take_along_axis(
                        tile, lane[k], axis=1
                    )
            value = {}
            for k in range(8):
                for j in range(k, 8):
                    value[j, k] = jnp.broadcast_to(
                        small[8 * k + j:8 * k + j + 1, :], (8, HALF)
                    )
            small[64:72, :] = head
            small[72:80, :] = work[pl.ds(top, 8), HALF:2 * HALF]
            row = [
                [
                    jnp.broadcast_to(small[64 + 8 * part + k:65 + 8 * part + k, :], (8, HALF))
                    for part in range(2)
                ]
                for k in range(8)
            ]
            factor = {}
            recip = []
            for k in range(8):
                recip.append(1.0 / value[k, k])
                for j in range(k + 1, 8):
                    factor[j, k] = value[j, k] * recip[k]
                for j in range(k + 1, 8):
                    for i in range(j, 8):
                        value[i, j] = value[i, j] - factor[j, k] * value[i, k]
                    for part in range(2):
                        row[j][part] = row[j][part] - factor[j, k] * row[k][part]
            ids = lax.broadcasted_iota(jnp.int32, (8, HALF), 0)
            kept = [row[0][1], value[0, 0], recip[0]]
            for k in range(1, 8):
                kept[0] = jnp.where(ids == k, row[k][1], kept[0])
                kept[1] = jnp.where(ids == k, value[k, k], kept[1])
                kept[2] = jnp.where(ids == k, recip[k], kept[2])
            inverse[pl.ds(top, 8), :] = kept[0]
            pivots[pl.ds(top, 8), :] = kept[1]
            recips[pl.ds(top, 8), :] = kept[2]
            for k in range(7, -1, -1):
                for part in range(2):
                    total = row[k][part] * recip[k]
                    for j in range(k + 1, 8):
                        total = total - factor[j, k] * row[j][part]
                    row[k][part] = total
            for i in range(first, 16):
                for part in range(2):
                    at = (slice(8 * i, 8 * i + 8), slice(part * HALF, (part + 1) * HALF))
                    total = work[at]
                    for k in range(8):
                        total = total - (
                            columns[8 * (8 * i + k):8 * (8 * i + k) + 8, :] * row[k][part]
                        )
                    work[at] = total
            return carry

        return step

    for quarter in range(4):
        lax.fori_loop(quarter * 4, quarter * 4 + 4, panel(quarter * 4), 0)


def factor(square, order, work, inverse, pivots, recips, columns, small):
    size = square.shape[0]
    ids = lax.broadcasted_iota(jnp.int32, (size, size), 0)
    chosen = (ids == order).astype(F32)
    moved = times(chosen, times(square, chosen, NN, EXACT), TN, EXACT)
    eye = (
        lax.broadcasted_iota(jnp.int32, (HALF, HALF), 0)
        == lax.broadcasted_iota(jnp.int32, (HALF, HALF), 1)
    ).astype(F32)
    lo, hi = slice(0, HALF), slice(HALF, 2 * HALF)
    work[:, lo] = moved[lo, lo]
    work[:, hi] = eye
    eliminate(work, inverse.at[lo], pivots.at[lo], recips.at[lo], columns, small)
    first = inverse[lo, :]
    upper = times(first, moved[lo, hi], NN, EXACT)
    scaled = upper * recips[lo, :]
    work[:, lo] = moved[hi, hi] - times(scaled, upper, TN, EXACT)
    work[:, hi] = eye
    below = times(scaled, first, TN, EXACT)
    eliminate(work, inverse.at[hi], pivots.at[hi], recips.at[hi], columns, small)
    second = inverse[hi, :]
    cross = -times(second, below, NN, EXACT)
    top = jnp.concatenate([first * recips[lo, :], jnp.zeros((HALF, HALF), F32)], axis=1)
    low = jnp.concatenate([cross * recips[hi, :], second * recips[hi, :]], axis=1)
    solver = times(jnp.concatenate([top, low], axis=0), chosen, NT, EXACT)
    values = jnp.concatenate([pivots[lo, :].T[0:1, :], pivots[hi, :].T[0:1, :]], axis=1)
    return solver, values


def panels_kernel(whole, rows, cols, corner, prev_pivots, orders, left, right, pivot_rows, front, landed, *scratch):
    g, r, c = place()

    @pl.when(c == 0)
    def _():
        lo, hi = slice(0, WIDTH), slice(WIDTH, 2 * WIDTH)
        fetch = pltpu.make_async_copy(whole.at[:, 0:2 * WIDTH], front, landed)
        fetch.start()
        near = cols[0:2 * WIDTH, :]
        before = prev_pivots[...]
        near_scaled = (near.astype(F32) * before).astype(BF16)
        rows_scaled = (rows[...].astype(F32) * before).astype(BF16)
        both = times(near_scaled[lo], near[lo], NT) + times(near[lo], near_scaled[lo], NT)
        solver, values = factor(corner[lo, lo] - 0.5 * both, orders[0:1, :], *scratch)
        pivot_rows[0:1, :] = values
        fetch.wait()
        panel = front[:, lo] - times(rows_scaled, near[lo], NT)
        shown = times(panel, solver, NT, EXACT).astype(BF16)
        left[...] = shown
        edge = corner[hi, lo] - times(near_scaled[hi], near[lo], NT)
        edge = times(edge, solver, NT, EXACT).astype(BF16)
        edge_scaled = (edge.astype(F32) * values).astype(BF16)
        both = times(near_scaled[hi], near[hi], NT) + times(near[hi], near_scaled[hi], NT)
        more = times(edge_scaled, edge, NT) + times(edge, edge_scaled, NT)
        square = (corner[hi, hi] - 0.5 * both) - 0.5 * more
        solver, later = factor(square, orders[1:2, :], *scratch)
        pivot_rows[1:2, :] = later
        shown_scaled = (shown.astype(F32) * values).astype(BF16)
        panel = front[:, hi] - times(rows_scaled, near[hi], NT)
        panel = panel - times(shown_scaled, edge, NT)
        right[...] = times(panel, solver, NT, EXACT).astype(BF16)


def body(front, prev_lower, prev_pivots, pivot_order):
    row_count, col_count = front.shape
    width = prev_lower.shape[1]
    g, r, c = place()
    vmem = pl.BlockSpec(memory_space=pltpu.VMEM)
    shape = jax.ShapeDtypeStruct
    dma = pltpu.SemaphoreType.DMA
    rows, cols, corner = pl.pallas_call(
        gather_kernel,
        out_shape=[
            shape((row_count, width), BF16),
            shape((col_count, width), BF16),
            shape((2 * width, 2 * width), F32),
        ],
        in_specs=[vmem, pl.BlockSpec(memory_space=pl.ANY)],
        out_specs=[vmem] * 3,
        scratch_shapes=Spread.semaphores() + Corner.semaphores(),
        compiler_params=pltpu.CompilerParams(
            collective_id=0, has_side_effects=True, vmem_limit_bytes=VMEM_LIMIT
        ),
        name="gather",
    )(prev_lower, front)
    left, right, pivot_rows = pl.pallas_call(
        panels_kernel,
        out_shape=[
            shape((row_count, width), BF16),
            shape((row_count, width), BF16),
            shape((2, width), F32),
        ],
        in_specs=[pl.BlockSpec(memory_space=pl.ANY)] + [vmem] * 5,
        out_specs=[vmem] * 3,
        scratch_shapes=[
            pltpu.VMEM((row_count, 2 * width), F32),
            dma,
            pltpu.VMEM((HALF, 2 * HALF), F32),
            pltpu.VMEM((2 * HALF, HALF), F32),
            pltpu.VMEM((2 * HALF, HALF), F32),
            pltpu.VMEM((2 * HALF, HALF), F32),
            pltpu.VMEM((8 * HALF, HALF), F32),
            pltpu.VMEM((80, HALF), F32),
        ],
        compiler_params=pltpu.CompilerParams(vmem_limit_bytes=VMEM_LIMIT),
        name="panels",
    )(front, rows, cols, corner, prev_pivots.reshape(1, width), pivot_order)
    chunk, second, shared, new_rows, new_cols = pl.pallas_call(
        share_kernel,
        out_shape=[
            shape((CHUNK, width), BF16),
            shape((CHUNK, width), BF16),
            shape((2, width), F32),
            shape((row_count, width), BF16),
            shape((col_count, width), BF16),
        ],
        in_specs=[vmem] * 3,
        out_specs=[vmem] * 5,
        scratch_shapes=Spread.semaphores() + [dma((3, 16)), dma((3,)), dma((3,))],
        compiler_params=pltpu.CompilerParams(
            collective_id=1, has_side_effects=True, vmem_limit_bytes=VMEM_LIMIT
        ),
        name="share",
    )(left, right, pivot_rows)

    first_row = (g * 16 + r) * row_count
    row_ids = first_row + lax.broadcasted_iota(jnp.int32, (row_count, 1), 0)
    col_ids = c * col_count + lax.broadcasted_iota(jnp.int32, (col_count, 1), 0)
    own_ids = first_row + c * CHUNK + lax.broadcasted_iota(jnp.int32, (CHUNK, 1), 0)
    none = jnp.zeros((), BF16)
    new_rows = jnp.where(row_ids >= width, new_rows, none)
    new_cols = jnp.where(col_ids >= width, new_cols, none)
    second = jnp.where(own_ids >= width, second, none)
    scaled = jnp.concatenate(
        [
            (rows.astype(F32) * prev_pivots).astype(BF16),
            (new_rows.astype(F32) * shared[0]).astype(BF16),
        ],
        axis=1,
    )
    schur = front - times(scaled, jnp.concatenate([cols, new_cols], axis=1), NT)
    panels = jnp.concatenate([chunk.astype(F32) * shared[0], second.astype(F32) * shared[1]], axis=1)
    return schur, panels, shared.reshape(2 * width)


def solution(mesh):
    in_specs = (P(("grp", "row"), "col"), P(("grp", "row", "col"), None), P(), P())
    out_specs = (P(("grp", "row"), "col"), P(("grp", "row", "col"), None), P())
    return jax.shard_map(body, mesh=mesh, in_specs=in_specs, out_specs=out_specs, check_vma=False)
```

```python
import jax
import jax.numpy as jnp
from jax import lax
from jax.experimental import pallas as pl
from jax.experimental.pallas import tpu as pltpu
from jax.sharding import PartitionSpec as P

F32 = jnp.float32
BF16 = jnp.bfloat16
EXACT = lax.Precision.HIGHEST
MESH = pl.DeviceIdType.MESH
CHUNK = 32
WIDTH = 256
HALF = 128
VMEM_LIMIT = 60 * 1024 * 1024


def place():
    return lax.axis_index("grp"), lax.axis_index("row"), lax.axis_index("col")


def remote(src, dst, send_sem, recv_sem, device):
    return pltpu.make_async_remote_copy(
        src_ref=src, dst_ref=dst, send_sem=send_sem, recv_sem=recv_sem,
        device_id=device, device_id_type=MESH,
    )


def signal(barrier, device):
    pl.semaphore_signal(barrier, inc=1, device_id=device, device_id_type=MESH)


def turn(value, step, size):
    return lax.rem(value + step + size, size)


def block(ref, number, rows):
    return ref.at[pl.ds(pl.multiple_of(number * rows, rows), rows)]


class Spread:
    def __init__(self, chunk, rows, cols, sems, full=None):
        self.chunk, self.rows, self.cols, self.full = chunk, rows, cols, full
        (self.zs, self.zr, self.fs, self.fr, self.ps, self.pr,
         self.xs, self.xr, self.cs, self.cr, self.own) = sems
        g, r, c = place()
        self.g, self.r, self.c = g, r, c
        self.x, self.yh, self.yl, self.z = r // 4, r % 4, c // 8, c % 8

    @staticmethod
    def semaphores():
        dma = pltpu.SemaphoreType.DMA
        return [dma((7,)), dma((7,)), dma((8,)), dma((8,)), dma((4,)), dma((4,)),
                dma((3,)), dma((3,)), dma((4,)), dma((4,)), dma((2,))]

    def target(self, j):
        return (self.r % 2, (self.c // 4) * 4 + j, self.g * 8 + self.r // 2)

    def source(self, i):
        return (self.c // 8, (2 * self.c + self.g) % 16, self.x * 4 + i)

    def is_me(self, device):
        return (device[0] == self.g) & (device[1] == self.r) & (device[2] == self.c)

    def greet(self, barrier):
        g, r, c = self.g, self.r, self.c
        for dz in range(1, 8):
            signal(barrier, (g, r, self.yl * 8 + turn(self.z, -dz, 8)))
        signal(barrier, (g, r, (1 - self.yl) * 8 + self.z))
        for dx in range(1, 4):
            signal(barrier, (g, turn(self.x, -dx, 4) * 4 + self.yh, c))
        signal(barrier, (1 - g, r, c))
        count = jnp.int32(12)
        for i in range(4):
            source = self.source(i)

            @pl.when(jnp.logical_not(self.is_me(source)))
            def _():
                signal(barrier, source)

            count += jnp.where(self.is_me(self.target(i)), 0, 1)
        return count

    def crossing(self, j):
        slot = (self.r % 2) * 16 + self.c
        return remote(self.chunk, block(self.cols, slot, CHUNK), self.ps.at[j],
                      self.pr.at[self.c % 4], self.target(j))

    def arriving(self, i):
        slot = self.g * 16 + self.x * 4 + i
        return remote(self.chunk, block(self.cols, slot, CHUNK), self.ps.at[i],
                      self.pr.at[i], self.source(i))

    def crossing_own(self):
        slot = (self.r % 2) * 16 + self.c
        return pltpu.make_async_copy(self.chunk, block(self.cols, slot, CHUNK), self.own.at[0])

    def across_z(self, dz, slot_z):
        return remote(self.chunk, block(self.rows, self.yl * 8 + slot_z, CHUNK),
                      self.zs.at[dz - 1], self.zr.at[dz - 1],
                      (self.g, self.r, self.yl * 8 + turn(self.z, dz, 8)))

    def partner(self, dz, side):
        slot = side * 8 + turn(self.z, -dz, 8)
        held = self.rows if self.full is None else self.full
        src = self.chunk if dz == 0 else block(held, slot, CHUNK)
        return remote(src, block(self.rows, slot, CHUNK), self.fs.at[dz], self.fr.at[dz],
                      (self.g, self.r, (1 - self.yl) * 8 + self.z))

    def across_x(self, dx, x):
        part = block(self.cols, self.g * 4 + x, 4 * CHUNK)
        return remote(part, part, self.xs.at[dx - 1], self.xr.at[dx - 1],
                      (self.g, turn(self.x, dx, 4) * 4 + self.yh, self.c))

    def sibling(self, dx, grp):
        part = block(self.cols, grp * 4 + turn(self.x, -dx, 4), 4 * CHUNK)
        return remote(part, part, self.cs.at[dx], self.cr.at[dx], (1 - self.g, self.r, self.c))

    def own_row_copy(self):
        return pltpu.make_async_copy(self.chunk, block(self.rows, self.c, CHUNK), self.own.at[1])

    def begin(self):
        for j in range(4):
            me = self.is_me(self.target(j))

            @pl.when(me)
            def _():
                self.crossing_own().start()

            @pl.when(jnp.logical_not(me))
            def _():
                self.crossing(j).start()

        for dz in range(1, 8):
            self.across_z(dz, self.z).start()
        for dz in range(1 if self.full is None else 8):
            self.partner(dz, self.yl).start()
        self.own_row_copy().start()

    def first_columns(self):
        for i in range(4):
            me = self.is_me(self.source(i))

            @pl.when(me)
            def _():
                self.crossing_own().wait()

            @pl.when(jnp.logical_not(me))
            def _():
                self.arriving(i).wait_recv()

        for dx in range(1, 4):
            self.across_x(dx, self.x).start()
        self.sibling(0, self.g).start()

    def pass_rows(self):
        for dz in range(1, 8):
            self.across_z(dz, turn(self.z, -dz, 8)).wait_recv()
            if self.full is None:
                self.partner(dz, self.yl).start()

    def pass_columns(self):
        for dx in range(1, 4):
            self.across_x(dx, turn(self.x, -dx, 4)).wait_recv()
            self.sibling(dx, self.g).start()

    def finish(self):
        self.own_row_copy().wait()
        for dz in range(8):
            self.partner(dz, 1 - self.yl).wait_recv()
        for dx in range(4):
            self.sibling(dx, 1 - self.g).wait_recv()

    def drain(self):
        for j in range(4):
            @pl.when(jnp.logical_not(self.is_me(self.target(j))))
            def _():
                self.crossing(j).wait_send()

        for dz in range(1, 8):
            self.across_z(dz, self.z).wait_send()
        for dz in range(8):
            self.partner(dz, self.yl).wait_send()
        for dx in range(1, 4):
            self.across_x(dx, self.x).wait_send()
        for dx in range(4):
            self.sibling(dx, self.g).wait_send()


class Corner:
    def __init__(self, front, first, corner, sems):
        self.front, self.first, self.corner = front, first, corner
        self.ts, self.tr, self.ys, self.yr, self.xs, self.xr, self.cs, self.cr = sems
        self.g, self.r, self.c = place()
        self.x, self.yh = self.r // 4, self.r % 4
        self.q = self.g * 16 + self.r
        self.rows = corner.shape[0] // 32
        self.lanes = corner.shape[1]

    @staticmethod
    def semaphores():
        dma = pltpu.SemaphoreType.DMA
        return [dma((32,)), dma, dma((3,)), dma((3,)), dma((3,)), dma((3,)), dma((4,)), dma((4,))]

    def greet(self, barrier):
        @pl.when(self.c == 0)
        def _():
            for dy in range(1, 4):
                signal(barrier, (self.g, self.x * 4 + turn(self.yh, -dy, 4), self.c))

            @pl.when(self.q != 0)
            def _():
                signal(barrier, (0, 0, 0))

        return jnp.where(self.c == 0, 3, 0) + jnp.where((self.q == 0) & (self.c == 0), 31, 0)

    def piece(self, slot):
        start = pl.multiple_of(self.first + slot * self.rows, self.rows)
        return self.front.at[pl.ds(start, self.rows), pl.ds(0, self.lanes)]

    def handing(self, slot):
        return remote(self.piece(slot), block(self.corner, slot, self.rows), self.ts.at[slot],
                      self.tr, (slot // 16, slot % 16, 0))

    def keeping(self):
        return pltpu.make_async_copy(self.piece(0), block(self.corner, 0, self.rows), self.tr)

    def across_y(self, dy, yh):
        part = block(self.corner, self.g * 16 + self.x * 4 + yh, self.rows)
        return remote(part, part, self.ys.at[dy - 1], self.yr.at[dy - 1],
                      (self.g, self.x * 4 + turn(self.yh, dy, 4), self.c))

    def across_x(self, dx, x):
        part = block(self.corner, self.g * 4 + x, 4 * self.rows)
        return remote(part, part, self.xs.at[dx - 1], self.xr.at[dx - 1],
                      (self.g, turn(self.x, dx, 4) * 4 + self.yh, self.c))

    def sibling(self, dx, grp):
        part = block(self.corner, grp * 4 + turn(self.x, -dx, 4), 4 * self.rows)
        return remote(part, part, self.cs.at[dx], self.cr.at[dx], (1 - self.g, self.r, self.c))

    def begin(self):
        @pl.when((self.q == 0) & (self.c == 0))
        def _():
            self.keeping().start()

            @pl.loop(1, 32)
            def _(slot):
                self.handing(slot).start()

    def first_hop(self):
        @pl.when(self.q == 0)
        def _():
            self.keeping().wait()

        @pl.when(self.q != 0)
        def _():
            self.handing(self.q).wait_recv()

        for dy in range(1, 4):
            self.across_y(dy, self.yh).start()

    def second_hop(self):
        for dy in range(1, 4):
            self.across_y(dy, turn(self.yh, -dy, 4)).wait_recv()
        for dx in range(1, 4):
            self.across_x(dx, self.x).start()
        self.sibling(0, self.g).start()

    def third_hop(self):
        for dx in range(1, 4):
            self.across_x(dx, turn(self.x, -dx, 4)).wait_recv()
            self.sibling(dx, self.g).start()

    def finish(self):
        for dx in range(4):
            self.sibling(dx, 1 - self.g).wait_recv()

    def drain(self):
        @pl.when(self.q == 0)
        def _():
            @pl.loop(1, 32)
            def _(slot):
                self.handing(slot).wait_send()

        for dy in range(1, 4):
            self.across_y(dy, self.yh).wait_send()
        for dx in range(1, 4):
            self.across_x(dx, self.x).wait_send()
        for dx in range(4):
            self.sibling(dx, self.g).wait_send()


def times(a, b, dims, precision=None):
    return lax.dot_general(
        a, b, (dims, ((), ())), precision=precision, preferred_element_type=F32
    )


NN = ((1,), (0,))
NT = ((1,), (1,))
TN = ((0,), (0,))


def eliminate(work, inverse, pivots, recips, columns, small):
    def panel(first):
        def step(number, carry):
            top = pl.multiple_of(number * 8, 8)
            lane = [jnp.full((8, HALF), top + k, jnp.int32) for k in range(8)]
            head = work[pl.ds(top, 8), 0:HALF]
            for k in range(8):
                small[8 * k:8 * k + 8, :] = jnp.take_along_axis(head, lane[k], axis=1)
            for i in range(first, 16):
                tile = work[8 * i:8 * i + 8, 0:HALF]
                for k in range(8):
                    columns[8 * (8 * i + k):8 * (8 * i + k) + 8, :] = jnp.take_along_axis(
                        tile, lane[k], axis=1
                    )
            value = {}
            for k in range(8):
                for j in range(k, 8):
                    value[j, k] = jnp.broadcast_to(
                        small[8 * k + j:8 * k + j + 1, :], (8, HALF)
                    )
            small[64:72, :] = head
            small[72:80, :] = work[pl.ds(top, 8), HALF:2 * HALF]
            row = [
                [
                    jnp.broadcast_to(small[64 + 8 * part + k:65 + 8 * part + k, :], (8, HALF))
                    for part in range(2)
                ]
                for k in range(8)
            ]
            factor = {}
            recip = []
            for k in range(8):
                recip.append(1.0 / value[k, k])
                for j in range(k + 1, 8):
                    factor[j, k] = value[j, k] * recip[k]
                for j in range(k + 1, 8):
                    for i in range(j, 8):
                        value[i, j] = value[i, j] - factor[j, k] * value[i, k]
                    for part in range(2):
                        row[j][part] = row[j][part] - factor[j, k] * row[k][part]
            ids = lax.broadcasted_iota(jnp.int32, (8, HALF), 0)
            kept = [row[0][1], value[0, 0], recip[0]]
            for k in range(1, 8):
                kept[0] = jnp.where(ids == k, row[k][1], kept[0])
                kept[1] = jnp.where(ids == k, value[k, k], kept[1])
                kept[2] = jnp.where(ids == k, recip[k], kept[2])
            inverse[pl.ds(top, 8), :] = kept[0]
            pivots[pl.ds(top, 8), :] = kept[1]
            recips[pl.ds(top, 8), :] = kept[2]
            for k in range(7, -1, -1):
                for part in range(2):
                    total = row[k][part] * recip[k]
                    for j in range(k + 1, 8):
                        total = total - factor[j, k] * row[j][part]
                    row[k][part] = total
            for i in range(first, 16):
                for part in range(2):
                    at = (slice(8 * i, 8 * i + 8), slice(part * HALF, (part + 1) * HALF))
                    total = work[at]
                    for k in range(8):
                        total = total - (
                            columns[8 * (8 * i + k):8 * (8 * i + k) + 8, :] * row[k][part]
                        )
                    work[at] = total
            return carry

        return step

    for quarter in range(4):
        lax.fori_loop(quarter * 4, quarter * 4 + 4, panel(quarter * 4), 0)


def factor(square, order, halfway, work, inverse, pivots, recips, columns, small):
    size = square.shape[0]
    ids = lax.broadcasted_iota(jnp.int32, (size, size), 0)
    chosen = (ids == order).astype(F32)
    moved = times(chosen, times(square, chosen, NN, EXACT), TN, EXACT)
    eye = (
        lax.broadcasted_iota(jnp.int32, (HALF, HALF), 0)
        == lax.broadcasted_iota(jnp.int32, (HALF, HALF), 1)
    ).astype(F32)
    lo, hi = slice(0, HALF), slice(HALF, 2 * HALF)
    work[:, lo] = moved[lo, lo]
    work[:, hi] = eye
    eliminate(work, inverse.at[lo], pivots.at[lo], recips.at[lo], columns, small)
    halfway()
    first = inverse[lo, :]
    upper = times(first, moved[lo, hi], NN, EXACT)
    scaled = upper * recips[lo, :]
    work[:, lo] = moved[hi, hi] - times(scaled, upper, TN, EXACT)
    work[:, hi] = eye
    below = times(scaled, first, TN, EXACT)
    eliminate(work, inverse.at[hi], pivots.at[hi], recips.at[hi], columns, small)
    second = inverse[hi, :]
    cross = -times(second, below, NN, EXACT)
    top = jnp.concatenate([first * recips[lo, :], jnp.zeros((HALF, HALF), F32)], axis=1)
    low = jnp.concatenate([cross * recips[hi, :], second * recips[hi, :]], axis=1)
    solver = times(jnp.concatenate([top, low], axis=0), chosen, NT, EXACT)
    values = jnp.concatenate([pivots[lo, :].T[0:1, :], pivots[hi, :].T[0:1, :]], axis=1)
    return solver, values


def window_kernel(
    prev_chunk, whole, prev_pivots, orders,
    left_side, right_side, panels, pivots_out,
    rows, cols, new_rows, new_cols, chunk, second, shared,
    left, right, values, corner, edges, front, landed,
    work, inverse, pivots, recips, columns, small,
    send, recv, *sems,
):
    g, r, c = place()
    q = g * 16 + r
    split = len(Spread.semaphores())
    deal = len(Corner.semaphores())
    old = Spread(prev_chunk, rows, cols, sems[:split])
    top_square = Corner(whole, 0, corner, sems[2 * split:2 * split + deal])
    low_square = Corner(whole, WIDTH, edges, sems[2 * split + deal:])
    scratch = (work, inverse, pivots, recips, columns, small)
    lo, hi = slice(0, WIDTH), slice(WIDTH, 2 * WIDTH)

    def handed(number, panel, to):
        device = (g, r, to)
        if number == 0:
            source, landing = block((left, right)[panel], to, CHUNK), (chunk, second)[panel]
        else:
            source, landing = values.at[panel], shared.at[panel]
        return remote(source, landing, send.at[2 * number + panel, to],
                      recv.at[2 * number + panel], device)

    barrier = pltpu.get_barrier_semaphore()
    count = old.greet(barrier) + top_square.greet(barrier)

    @pl.when(c != 0)
    def _():
        signal(barrier, (g, r, 0))

    pl.semaphore_wait(barrier, count + jnp.where(c == 0, 15, 0))
    top_square.begin()
    old.begin()
    low_square.begin()
    fetch = pltpu.make_async_copy(whole.at[:, 0:2 * WIDTH], front, landed)

    @pl.when(c == 0)
    def _():
        fetch.start()
        top_square.first_hop()

    old.pass_rows()
    old.first_columns()

    @pl.when(c == 0)
    def _():
        top_square.second_hop()

    old.pass_columns()

    @pl.when(c == 0)
    def _():
        top_square.third_hop()
        low_square.first_hop()

    old.finish()
    before = prev_pivots[...]
    rows_scaled = (rows[...].astype(F32) * before).astype(BF16)
    left_side[:, lo] = rows_scaled
    right_side[:, lo] = cols[...]

    @pl.when(c == 0)
    def _():
        new = Spread(block(left, 0, CHUNK), new_rows, new_cols, sems[split:2 * split], left)
        near = cols[0:2 * WIDTH, :]
        near_scaled = (near.astype(F32) * before).astype(BF16)
        both = times(near_scaled[lo], near[lo], NT) + times(near[lo], near_scaled[lo], NT)
        top_square.finish()
        solver, given = factor(
            corner[...] - 0.5 * both, orders[0:1, :], low_square.second_hop, *scratch
        )
        values[0] = jnp.broadcast_to(given, (8, WIDTH))
        fetch.wait()
        panel = front[:, lo] - times(left_side[:, lo], near[lo], NT)
        shown = times(panel, solver, NT, EXACT).astype(BF16)
        left[...] = shown
        low_square.third_hop()
        low_square.finish()
        edge = edges[:, lo] - times(near_scaled[hi], near[lo], NT)
        edge = times(edge, solver, NT, EXACT).astype(BF16)
        for to in range(1, 16):
            handed(0, 0, to).start()
        new.begin()
        for to in range(1, 16):
            handed(1, 0, to).start()
        chunk[...] = left[0:CHUNK, :]
        edge_scaled = (edge.astype(F32) * given).astype(BF16)
        both = times(near_scaled[hi], near[hi], NT) + times(near[hi], near_scaled[hi], NT)
        more = times(edge_scaled, edge, NT) + times(edge, edge_scaled, NT)
        square = (edges[:, hi] - 0.5 * both) - 0.5 * more
        solver, later = factor(square, orders[1:2, :], lambda: None, *scratch)
        values[1] = jnp.broadcast_to(later, (8, WIDTH))
        shown_scaled = (left[...].astype(F32) * given).astype(BF16)
        panel = front[:, hi] - times(left_side[:, lo], near[hi], NT)
        panel = panel - times(shown_scaled, edge, NT)
        right[...] = times(panel, solver, NT, EXACT).astype(BF16)
        new.first_columns()
        for to in range(1, 16):
            handed(1, 1, to).start()
            handed(0, 1, to).start()
        second[...] = right[0:CHUNK, :]
        shared[...] = values[...]
        new.pass_rows()
        new.pass_columns()
        new.finish()
        new.drain()
        for to in range(1, 16):
            for panel in range(2):
                handed(0, panel, to).wait_send()
                handed(1, panel, to).wait_send()
        top_square.drain()
        low_square.drain()

    @pl.when(c != 0)
    def _():
        new = Spread(chunk, new_rows, new_cols, sems[split:2 * split])
        handed(0, 0, c).wait_recv()
        new.begin()
        new.pass_rows()
        new.first_columns()
        new.pass_columns()
        handed(1, 0, c).wait_recv()
        handed(1, 1, c).wait_recv()
        handed(0, 1, c).wait_recv()
        new.finish()
        new.drain()

    old.drain()
    row_ids = q * rows.shape[0] + lax.broadcasted_iota(jnp.int32, (rows.shape[0], 1), 0)
    col_ids = c * cols.shape[0] + lax.broadcasted_iota(jnp.int32, (cols.shape[0], 1), 0)
    own_ids = q * rows.shape[0] + c * CHUNK + lax.broadcasted_iota(jnp.int32, (CHUNK, 1), 0)
    given, later = shared[0, 0:1, :], shared[1, 0:1, :]
    live = jnp.where(row_ids >= WIDTH, new_rows[...].astype(F32), 0.0)
    left_side[:, hi] = (live * given).astype(BF16)
    right_side[:, hi] = jnp.where(col_ids >= WIDTH, new_cols[...].astype(F32), 0.0).astype(BF16)
    panels[:, lo] = chunk[...].astype(F32) * given
    panels[:, hi] = jnp.where(own_ids >= WIDTH, second[...].astype(F32), 0.0) * later
    pivots_out[0:1, :] = given
    pivots_out[1:2, :] = later


def body(front, prev_lower, prev_pivots, pivot_order):
    row_count, col_count = front.shape
    width = prev_lower.shape[1]
    vmem = pl.BlockSpec(memory_space=pltpu.VMEM)
    shape = jax.ShapeDtypeStruct
    dma = pltpu.SemaphoreType.DMA
    left_side, right_side, panels, pivots = pl.pallas_call(
        window_kernel,
        out_shape=[
            shape((row_count, 2 * width), BF16),
            shape((col_count, 2 * width), BF16),
            shape((CHUNK, 2 * width), F32),
            shape((2, width), F32),
        ],
        in_specs=[vmem, pl.BlockSpec(memory_space=pl.ANY), vmem, vmem],
        out_specs=[vmem] * 4,
        scratch_shapes=[
            pltpu.VMEM((row_count, width), BF16),
            pltpu.VMEM((col_count, width), BF16),
            pltpu.VMEM((row_count, width), BF16),
            pltpu.VMEM((col_count, width), BF16),
            pltpu.VMEM((CHUNK, width), BF16),
            pltpu.VMEM((CHUNK, width), BF16),
            pltpu.VMEM((2, 8, width), F32),
            pltpu.VMEM((row_count, width), BF16),
            pltpu.VMEM((row_count, width), BF16),
            pltpu.VMEM((2, 8, width), F32),
            pltpu.VMEM((width, width), F32),
            pltpu.VMEM((width, 2 * width), F32),
            pltpu.VMEM((row_count, 2 * width), F32),
            dma,
            pltpu.VMEM((HALF, 2 * HALF), F32),
            pltpu.VMEM((2 * HALF, HALF), F32),
            pltpu.VMEM((2 * HALF, HALF), F32),
            pltpu.VMEM((2 * HALF, HALF), F32),
            pltpu.VMEM((8 * HALF, HALF), F32),
            pltpu.VMEM((80, HALF), F32),
            dma((4, 16)),
            dma((4,)),
        ]
        + Spread.semaphores() * 2
        + Corner.semaphores() * 2,
        compiler_params=pltpu.CompilerParams(
            collective_id=0, has_side_effects=True, vmem_limit_bytes=VMEM_LIMIT
        ),
        name="window",
    )(prev_lower, front, prev_pivots.reshape(1, width), pivot_order)
    schur = front - times(left_side, right_side, NT)
    return schur, panels, pivots.reshape(2 * width)


def solution(mesh):
    in_specs = (P(("grp", "row"), "col"), P(("grp", "row", "col"), None), P(), P())
    out_specs = (P(("grp", "row"), "col"), P(("grp", "row", "col"), None), P())
    return jax.shard_map(body, mesh=mesh, in_specs=in_specs, out_specs=out_specs, check_vma=False)
```

```python
import jax
import jax.numpy as jnp
from jax import lax
from jax.experimental import pallas as pl
from jax.experimental.pallas import tpu as pltpu
from jax.sharding import PartitionSpec as P

F32 = jnp.float32
BF16 = jnp.bfloat16
EXACT = lax.Precision.HIGHEST
MESH = pl.DeviceIdType.MESH
CHUNK = 32
WIDTH = 256
HALF = 128
VMEM_LIMIT = 60 * 1024 * 1024


def place():
    return lax.axis_index("grp"), lax.axis_index("row"), lax.axis_index("col")


def remote(src, dst, send_sem, recv_sem, device):
    return pltpu.make_async_remote_copy(
        src_ref=src, dst_ref=dst, send_sem=send_sem, recv_sem=recv_sem,
        device_id=device, device_id_type=MESH,
    )


def signal(barrier, device):
    pl.semaphore_signal(barrier, inc=1, device_id=device, device_id_type=MESH)


def turn(value, step, size):
    return lax.rem(value + step + size, size)


def block(ref, number, rows):
    return ref.at[pl.ds(pl.multiple_of(number * rows, rows), rows)]


class Spread:
    def __init__(self, chunk, rows, cols, sems, full=None):
        self.chunk, self.rows, self.cols, self.full = chunk, rows, cols, full
        (self.zs, self.zr, self.fs, self.fr, self.ps, self.pr,
         self.xs, self.xr, self.cs, self.cr, self.own) = sems
        g, r, c = place()
        self.g, self.r, self.c = g, r, c
        self.x, self.yh, self.yl, self.z = r // 4, r % 4, c // 8, c % 8

    @staticmethod
    def semaphores():
        dma = pltpu.SemaphoreType.DMA
        return [dma((7,)), dma((7,)), dma((8,)), dma((8,)), dma((4,)), dma((4,)),
                dma((3,)), dma((3,)), dma((4,)), dma((4,)), dma((2,))]

    def target(self, j):
        return (self.r % 2, (self.c // 4) * 4 + j, self.g * 8 + self.r // 2)

    def source(self, i):
        return (self.c // 8, (2 * self.c + self.g) % 16, self.x * 4 + i)

    def is_me(self, device):
        return (device[0] == self.g) & (device[1] == self.r) & (device[2] == self.c)

    def greet(self, barrier):
        g, r, c = self.g, self.r, self.c
        for dz in range(1, 8):
            signal(barrier, (g, r, self.yl * 8 + turn(self.z, -dz, 8)))
        signal(barrier, (g, r, (1 - self.yl) * 8 + self.z))
        for dx in range(1, 4):
            signal(barrier, (g, turn(self.x, -dx, 4) * 4 + self.yh, c))
        signal(barrier, (1 - g, r, c))
        count = jnp.int32(12)
        for i in range(4):
            source = self.source(i)

            @pl.when(jnp.logical_not(self.is_me(source)))
            def _():
                signal(barrier, source)

            count += jnp.where(self.is_me(self.target(i)), 0, 1)
        return count

    def crossing(self, j):
        slot = (self.r % 2) * 16 + self.c
        return remote(self.chunk, block(self.cols, slot, CHUNK), self.ps.at[j],
                      self.pr.at[self.c % 4], self.target(j))

    def arriving(self, i):
        slot = self.g * 16 + self.x * 4 + i
        return remote(self.chunk, block(self.cols, slot, CHUNK), self.ps.at[i],
                      self.pr.at[i], self.source(i))

    def crossing_own(self):
        slot = (self.r % 2) * 16 + self.c
        return pltpu.make_async_copy(self.chunk, block(self.cols, slot, CHUNK), self.own.at[0])

    def across_z(self, dz, slot_z):
        return remote(self.chunk, block(self.rows, self.yl * 8 + slot_z, CHUNK),
                      self.zs.at[dz - 1], self.zr.at[dz - 1],
                      (self.g, self.r, self.yl * 8 + turn(self.z, dz, 8)))

    def partner(self, dz, side):
        slot = side * 8 + turn(self.z, -dz, 8)
        held = self.rows if self.full is None else self.full
        src = self.chunk if dz == 0 else block(held, slot, CHUNK)
        return remote(src, block(self.rows, slot, CHUNK), self.fs.at[dz], self.fr.at[dz],
                      (self.g, self.r, (1 - self.yl) * 8 + self.z))

    def across_x(self, dx, x):
        part = block(self.cols, self.g * 4 + x, 4 * CHUNK)
        return remote(part, part, self.xs.at[dx - 1], self.xr.at[dx - 1],
                      (self.g, turn(self.x, dx, 4) * 4 + self.yh, self.c))

    def sibling(self, dx, grp):
        part = block(self.cols, grp * 4 + turn(self.x, -dx, 4), 4 * CHUNK)
        return remote(part, part, self.cs.at[dx], self.cr.at[dx], (1 - self.g, self.r, self.c))

    def own_row_copy(self):
        return pltpu.make_async_copy(self.chunk, block(self.rows, self.c, CHUNK), self.own.at[1])

    def begin(self):
        for j in range(4):
            me = self.is_me(self.target(j))

            @pl.when(me)
            def _():
                self.crossing_own().start()

            @pl.when(jnp.logical_not(me))
            def _():
                self.crossing(j).start()

        for dz in range(1, 8):
            self.across_z(dz, self.z).start()
        for dz in range(1 if self.full is None else 8):
            self.partner(dz, self.yl).start()
        self.own_row_copy().start()

    def columns_arrive(self):
        for i in range(4):
            me = self.is_me(self.source(i))

            @pl.when(me)
            def _():
                self.crossing_own().wait()

            @pl.when(jnp.logical_not(me))
            def _():
                self.arriving(i).wait_recv()

    def columns_send(self):
        for dx in range(1, 4):
            self.across_x(dx, self.x).start()
        self.sibling(0, self.g).start()

    def urgent(self, grp, dx):
        return (grp == 0) & (turn(self.x, -dx, 4) < 2)

    def pass_rows(self):
        for dz in range(1, 8):
            self.across_z(dz, turn(self.z, -dz, 8)).wait_recv()
            if self.full is None:
                self.partner(dz, self.yl).start()

    def pass_column(self, dx):
        self.across_x(dx, turn(self.x, -dx, 4)).wait_recv()
        self.sibling(dx, self.g).start()

    def pass_columns(self):
        for dx in range(1, 4):
            self.pass_column(dx)

    def finish_rows(self):
        self.own_row_copy().wait()
        for dz in range(8):
            self.partner(dz, 1 - self.yl).wait_recv()

    def finish_column(self, dx):
        self.sibling(dx, 1 - self.g).wait_recv()

    def finish_columns(self):
        for dx in range(4):
            self.finish_column(dx)

    def drain(self):
        for j in range(4):
            @pl.when(jnp.logical_not(self.is_me(self.target(j))))
            def _():
                self.crossing(j).wait_send()

        for dz in range(1, 8):
            self.across_z(dz, self.z).wait_send()
        for dz in range(8):
            self.partner(dz, self.yl).wait_send()
        for dx in range(1, 4):
            self.across_x(dx, self.x).wait_send()
        for dx in range(4):
            self.sibling(dx, self.g).wait_send()


class Corner:
    def __init__(self, front, first, corner, sems):
        self.front, self.first, self.corner = front, first, corner
        self.ts, self.tr, self.ys, self.yr, self.xs, self.xr, self.cs, self.cr = sems
        self.g, self.r, self.c = place()
        self.x, self.yh = self.r // 4, self.r % 4
        self.q = self.g * 16 + self.r
        self.rows = corner.shape[0] // 32
        self.lanes = corner.shape[1]

    @staticmethod
    def semaphores():
        dma = pltpu.SemaphoreType.DMA
        return [dma((32,)), dma, dma((3,)), dma((3,)), dma((3,)), dma((3,)), dma((4,)), dma((4,))]

    def greet(self, barrier):
        @pl.when(self.c == 0)
        def _():
            for dy in range(1, 4):
                signal(barrier, (self.g, self.x * 4 + turn(self.yh, -dy, 4), self.c))

            @pl.when(self.q != 0)
            def _():
                signal(barrier, (0, 0, 0))

        return jnp.where(self.c == 0, 3, 0) + jnp.where((self.q == 0) & (self.c == 0), 31, 0)

    def piece(self, slot):
        start = pl.multiple_of(self.first + slot * self.rows, self.rows)
        return self.front.at[pl.ds(start, self.rows), pl.ds(0, self.lanes)]

    def handing(self, slot):
        return remote(self.piece(slot), block(self.corner, slot, self.rows), self.ts.at[slot],
                      self.tr, (slot // 16, slot % 16, 0))

    def keeping(self):
        return pltpu.make_async_copy(self.piece(0), block(self.corner, 0, self.rows), self.tr)

    def across_y(self, dy, yh):
        part = block(self.corner, self.g * 16 + self.x * 4 + yh, self.rows)
        return remote(part, part, self.ys.at[dy - 1], self.yr.at[dy - 1],
                      (self.g, self.x * 4 + turn(self.yh, dy, 4), self.c))

    def across_x(self, dx, x):
        part = block(self.corner, self.g * 4 + x, 4 * self.rows)
        return remote(part, part, self.xs.at[dx - 1], self.xr.at[dx - 1],
                      (self.g, turn(self.x, dx, 4) * 4 + self.yh, self.c))

    def sibling(self, dx, grp):
        part = block(self.corner, grp * 4 + turn(self.x, -dx, 4), 4 * self.rows)
        return remote(part, part, self.cs.at[dx], self.cr.at[dx], (1 - self.g, self.r, self.c))

    def begin(self):
        @pl.when((self.q == 0) & (self.c == 0))
        def _():
            self.keeping().start()

            @pl.loop(1, 32)
            def _(slot):
                self.handing(slot).start()

    def first_hop(self):
        @pl.when(self.q == 0)
        def _():
            self.keeping().wait()

        @pl.when(self.q != 0)
        def _():
            self.handing(self.q).wait_recv()

        for dy in range(1, 4):
            self.across_y(dy, self.yh).start()

    def second_hop(self):
        for dy in range(1, 4):
            self.across_y(dy, turn(self.yh, -dy, 4)).wait_recv()
        for dx in range(1, 4):
            self.across_x(dx, self.x).start()
        self.sibling(0, self.g).start()

    def third_hop(self):
        for dx in range(1, 4):
            self.across_x(dx, turn(self.x, -dx, 4)).wait_recv()
            self.sibling(dx, self.g).start()

    def finish(self):
        for dx in range(4):
            self.sibling(dx, 1 - self.g).wait_recv()

    def drain(self):
        @pl.when(self.q == 0)
        def _():
            @pl.loop(1, 32)
            def _(slot):
                self.handing(slot).wait_send()

        for dy in range(1, 4):
            self.across_y(dy, self.yh).wait_send()
        for dx in range(1, 4):
            self.across_x(dx, self.x).wait_send()
        for dx in range(4):
            self.sibling(dx, self.g).wait_send()


def times(a, b, dims, precision=None):
    return lax.dot_general(
        a, b, (dims, ((), ())), precision=precision, preferred_element_type=F32
    )


NN = ((1,), (0,))
NT = ((1,), (1,))
TN = ((0,), (0,))


def inverted(value):
    guess = pl.reciprocal(value, approx=True)
    guess = guess * (2.0 - value * guess)
    return guess * (2.0 - value * guess)


def eliminate(work, inverse, pivots, recips, columns, small, between=None):
    parts = (slice(0, HALF), slice(HALF, 2 * HALF))
    ids = lax.broadcasted_iota(jnp.int32, (8, HALF), 0)

    def spread_lane(tile, lane):
        return jnp.broadcast_to(tile[:, lane:lane + 1], (8, HALF))

    for number in range(16):
        if between is not None and number == 8:
            between()
        top = 8 * number
        mine = slice(top, top + 8)
        at = 256 * (number % 2)
        head = work[mine, parts[0]]
        for k in range(8):
            small[at + 8 * k:at + 8 * k + 8, :] = spread_lane(head, top + k)
        for i in range(number + 1, 16):
            tile = work[8 * i:8 * i + 8, parts[0]]
            for k in range(8):
                columns[8 * (8 * i + k):8 * (8 * i + k) + 8, :] = spread_lane(tile, top + k)
        value = {}
        for k in range(8):
            for j in range(k, 8):
                value[j, k] = jnp.broadcast_to(
                    small[at + 8 * k + j:at + 8 * k + j + 1, :], (8, HALF)
                )
        row = [
            [
                jnp.broadcast_to(work[top + k:top + k + 1, part], (8, HALF)) for part in parts
            ]
            for k in range(8)
        ]
        factor = {}
        recip = []
        for k in range(8):
            recip.append(inverted(value[k, k]))
            for j in range(k + 1, 8):
                factor[j, k] = value[j, k] * recip[k]
            for j in range(k + 1, 8):
                for i in range(j, 8):
                    value[i, j] = value[i, j] - factor[j, k] * value[i, k]
                for part in range(2):
                    row[j][part] = row[j][part] - factor[j, k] * row[k][part]
        kept = [row[0][1], value[0, 0], recip[0]]
        for k in range(1, 8):
            kept[0] = jnp.where(ids == k, row[k][1], kept[0])
            kept[1] = jnp.where(ids == k, value[k, k], kept[1])
            kept[2] = jnp.where(ids == k, recip[k], kept[2])
        inverse[mine, :] = kept[0]
        pivots[mine, :] = kept[1]
        recips[mine, :] = kept[2]
        if number == 15:
            break
        for k in range(7, -1, -1):
            for part in range(2):
                total = row[k][part] * recip[k]
                for j in range(k + 1, 8):
                    total = total - factor[j, k] * row[j][part]
                row[k][part] = total
        for i in range(number + 1, 16):
            rows = slice(8 * i, 8 * i + 8)
            for part in range(2):
                terms = [
                    columns[8 * (8 * i + k):8 * (8 * i + k) + 8, :] * row[k][part]
                    for k in range(8)
                ]
                while len(terms) > 1:
                    terms = [x + y for x, y in zip(terms[::2], terms[1::2])]
                work[rows, parts[part]] = work[rows, parts[part]] - terms[0]


def factor(square, order, hooks, work, inverse, pivots, recips, columns, small):
    size = square.shape[0]
    ids = lax.broadcasted_iota(jnp.int32, (size, size), 0)
    chosen = (ids == order).astype(F32)
    moved = times(chosen, times(square, chosen, NN, EXACT), TN, EXACT)
    eye = (
        lax.broadcasted_iota(jnp.int32, (HALF, HALF), 0)
        == lax.broadcasted_iota(jnp.int32, (HALF, HALF), 1)
    ).astype(F32)
    lo, hi = slice(0, HALF), slice(HALF, 2 * HALF)
    work[:, lo] = moved[lo, lo]
    work[:, hi] = eye
    eliminate(work, inverse.at[lo], pivots.at[lo], recips.at[lo], columns, small)
    hooks[0]()
    first = inverse[lo, :]
    upper = times(first, moved[lo, hi], NN, EXACT)
    scaled = upper * recips[lo, :]
    work[:, lo] = moved[hi, hi] - times(scaled, upper, TN, EXACT)
    work[:, hi] = eye
    below = times(scaled, first, TN, EXACT)
    eliminate(work, inverse.at[hi], pivots.at[hi], recips.at[hi], columns, small, hooks[1])
    hooks[2]()
    second = inverse[hi, :]
    cross = -times(second, below, NN, EXACT)
    top = jnp.concatenate([first * recips[lo, :], jnp.zeros((HALF, HALF), F32)], axis=1)
    low = jnp.concatenate([cross * recips[hi, :], second * recips[hi, :]], axis=1)
    solver = times(jnp.concatenate([top, low], axis=0), chosen, NT, EXACT)
    values = jnp.concatenate([pivots[lo, :].T[0:1, :], pivots[hi, :].T[0:1, :]], axis=1)
    return solver, values


def nothing():
    pass


def window_kernel(
    chunk_in, whole, pivots_in, orders_in,
    old_left, old_right, new_left_out, new_right_out, panels_out, pivots_out,
    prev_chunk, prev_pivots, orders, panels, pivots_kept, given_in, rows, rows_scaled, cols, new_rows, new_left, new_cols, chunk, second, shared,
    left, right, values, corner, edges, front, landed, stored,
    work, inverse, pivots, recips, columns, small,
    send, recv, *sems,
):
    g, r, c = place()
    q = g * 16 + r
    split = len(Spread.semaphores())
    deal = len(Corner.semaphores())
    old = Spread(prev_chunk, rows, cols, sems[:split])
    top_square = Corner(whole, 0, corner, sems[2 * split:2 * split + deal])
    low_square = Corner(whole, WIDTH, edges, sems[2 * split + deal:])
    scratch = (work, inverse, pivots, recips, columns, small)
    lo, hi = slice(0, WIDTH), slice(WIDTH, 2 * WIDTH)
    inputs = [
        pltpu.make_async_copy(source, target, given_in.at[n])
        for n, (source, target) in enumerate(
            ((chunk_in, prev_chunk), (pivots_in, prev_pivots), (orders_in, orders))
        )
    ]
    for copy in inputs:
        copy.start()

    def handed(number, panel, to):
        device = (g, r, to)
        if number == 0:
            source, landing = block((left, right)[panel], to, CHUNK), (chunk, second)[panel]
        else:
            source, landing = values.at[panel], shared.at[panel]
        return remote(source, landing, send.at[2 * number + panel, to],
                      recv.at[2 * number + panel], device)

    def keep_old():
        rows_scaled[...] = (rows[...].astype(F32) * before).astype(BF16)

    keeping = (
        pltpu.make_async_copy(rows_scaled, old_left, stored.at[0]),
        pltpu.make_async_copy(cols, old_right, stored.at[1]),
    )
    keep_left = pltpu.make_async_copy(new_left, new_left_out, stored.at[2])
    keep_panels = pltpu.make_async_copy(panels, panels_out, stored.at[4])
    keep_pivots = pltpu.make_async_copy(pivots_kept, pivots_out, stored.at[5])
    keep_right = pltpu.make_async_copy(new_cols, new_right_out, stored.at[3])
    barrier = pltpu.get_barrier_semaphore()
    count = old.greet(barrier) + top_square.greet(barrier)

    @pl.when(c != 0)
    def _():
        signal(barrier, (g, r, 0))

    with jax.named_scope("barrier"):
        pl.semaphore_wait(barrier, count + jnp.where(c == 0, 15, 0))
    for copy in inputs:
        copy.wait()
    before = prev_pivots[...]
    top_square.begin()
    old.begin()
    low_square.begin()
    fetch = pltpu.make_async_copy(whole.at[:, 0:2 * WIDTH], front, landed)

    @pl.when(c == 0)
    def _():
        new = Spread(block(left, 0, CHUNK), new_rows, new_cols, sems[split:2 * split], left)
        fetch.start()
        with jax.named_scope("top_first"):
            top_square.first_hop()
        with jax.named_scope("columns_arrive"):
            old.columns_arrive()

        @pl.when(old.urgent(g, 0))
        def _():
            old.columns_send()

        with jax.named_scope("top_second"):
            top_square.second_hop()
        with jax.named_scope("columns_pass"):
            for dx in range(1, 4):
                @pl.when(old.urgent(g, dx))
                def _():
                    old.pass_column(dx)

        with jax.named_scope("top_third"):
            top_square.third_hop()
        with jax.named_scope("columns_finish"):
            for dx in range(4):
                @pl.when(old.urgent(1 - g, dx))
                def _():
                    old.finish_column(dx)

        @pl.when(jnp.logical_not(old.urgent(g, 0)))
        def _():
            old.columns_send()

        with jax.named_scope("low_first"):
            low_square.first_hop()
        near = cols[lo, :]
        near_scaled = (near.astype(F32) * before).astype(BF16)
        both = times(near_scaled, near, NT) + times(near, near_scaled, NT)
        with jax.named_scope("top_finish"):
            top_square.finish()

        def middle():
            with jax.named_scope("hook0"):
                low_square.second_hop()
                old.pass_rows()

        def late():
            with jax.named_scope("hook1"):
                for dx in range(1, 4):
                    @pl.when(jnp.logical_not(old.urgent(g, dx)))
                    def _():
                        old.pass_column(dx)

        def last():
            with jax.named_scope("hook2"):
                low_square.third_hop()

        with jax.named_scope("factor0"):
            solver, given = factor(
                corner[...] - 0.5 * both, orders[0:1, :], (middle, late, last), *scratch
            )
        values[0] = jnp.broadcast_to(given, (8, WIDTH))
        with jax.named_scope("wait_rows"):
            fetch.wait()
            old.finish_rows()
        with jax.named_scope("panel0"):
            keep_old()
            panel = front[:, lo] - times(rows_scaled[...], near, NT)
            shown = times(panel, solver, NT, EXACT).astype(BF16)
            left[...] = shown
        with jax.named_scope("wait_low"):
            for dx in range(4):
                @pl.when(jnp.logical_not(old.urgent(1 - g, dx)))
                def _():
                    old.finish_column(dx)

            low_square.finish()
        with jax.named_scope("edge"):
            next_near = cols[hi, :]
            next_scaled = (next_near.astype(F32) * before).astype(BF16)
            edge = edges[:, lo] - times(next_scaled, near, NT)
            edge = times(edge, solver, NT, EXACT).astype(BF16)
        with jax.named_scope("scatter"):
            for to in range(1, 16):
                handed(0, 0, to).start()
            new.begin()
            for to in range(1, 16):
                handed(1, 0, to).start()
            for copy in keeping:
                copy.start()
        edge_scaled = (edge.astype(F32) * given).astype(BF16)
        both = times(next_scaled, next_near, NT) + times(next_near, next_scaled, NT)
        more = times(edge_scaled, edge, NT) + times(edge, edge_scaled, NT)
        square = (edges[:, hi] - 0.5 * both) - 0.5 * more

        def early_columns():
            with jax.named_scope("hook3"):
                new.columns_arrive()
                new.columns_send()

        def late_columns():
            with jax.named_scope("hook4"):
                new.pass_rows()

        with jax.named_scope("factor1"):
            solver, later = factor(
                square, orders[1:2, :], (nothing, early_columns, late_columns), *scratch
            )
        values[1] = jnp.broadcast_to(later, (8, WIDTH))
        with jax.named_scope("panel1"):
            shown_scaled = (left[...].astype(F32) * given).astype(BF16)
            panel = front[:, hi] - times(rows_scaled[...], next_near, NT)
            panel = panel - times(shown_scaled, edge, NT)
            right[...] = times(panel, solver, NT, EXACT).astype(BF16)
        @pl.when(q != 0)
        def _():
            new_left[...] = shown_scaled

        @pl.when(q == 0)
        def _():
            new_left[lo, :] = jnp.zeros_like(new_left[lo, :])
            new_left[hi, :] = shown_scaled[hi]

        chunk[...] = left[0:CHUNK, :]
        shared[...] = values[...]
        for to in range(1, 16):
            handed(1, 1, to).start()
            handed(0, 1, to).start()
        second[...] = right[0:CHUNK, :]
        with jax.named_scope("last_columns"):
            new.pass_columns()
        keep_left.start()
        with jax.named_scope("finish"):
            new.finish_rows()
            new.finish_columns()
        with jax.named_scope("drain"):
            new.drain()
        new_cols[lo, :] = jnp.zeros((WIDTH, WIDTH), BF16)

    @pl.when(c != 0)
    def _():
        with jax.named_scope("old"):
            old.pass_rows()
            old.columns_arrive()
            old.columns_send()
            old.pass_columns()
            old.finish_rows()
            old.finish_columns()
        keep_old()
        for copy in keeping:
            copy.start()
        new = Spread(chunk, new_rows, new_cols, sems[split:2 * split])
        with jax.named_scope("recv_chunk"):
            handed(0, 0, c).wait_recv()
        new.begin()
        with jax.named_scope("pass_rows"):
            new.pass_rows()
        with jax.named_scope("columns_arrive"):
            new.columns_arrive()
            new.columns_send()
        with jax.named_scope("pass_columns"):
            new.pass_columns()
        with jax.named_scope("finish_rows"):
            new.finish_rows()
            handed(1, 0, c).wait_recv()
        given = shared[0, 0:1, :]

        @pl.when(q != 0)
        def _():
            new_left[...] = (new_rows[...].astype(F32) * given).astype(BF16)

        @pl.when(q == 0)
        def _():
            new_left[lo, :] = jnp.zeros_like(new_left[lo, :])
            new_left[hi, :] = (new_rows[hi, :].astype(F32) * given).astype(BF16)

        keep_left.start()
        with jax.named_scope("finish_columns"):
            new.finish_columns()
        keep_right.start()
        with jax.named_scope("recv_values"):
            handed(1, 1, c).wait_recv()
            handed(0, 1, c).wait_recv()
        new.drain()

    given, later = shared[0, 0:1, :], shared[1, 0:1, :]
    panels[:, lo] = chunk[...].astype(F32) * given
    live = (q != 0) | (c >= WIDTH // CHUNK)

    @pl.when(live)
    def _():
        panels[:, hi] = second[...].astype(F32) * later

    @pl.when(jnp.logical_not(live))
    def _():
        panels[:, hi] = jnp.zeros((CHUNK, WIDTH), F32)

    pivots_kept[:, lo] = given
    pivots_kept[:, hi] = later
    keep_panels.start()
    keep_pivots.start()
    @pl.when(c == 0)
    def _():
        keep_right.start()
        with jax.named_scope("drain_last"):
            for to in range(1, 16):
                for panel in range(2):
                    handed(0, panel, to).wait_send()
                    handed(1, panel, to).wait_send()
            top_square.drain()
            low_square.drain()

    with jax.named_scope("drain_old"):
        old.drain()
        for copy in (*keeping, keep_left, keep_right, keep_panels, keep_pivots):
            copy.wait()


def apply_kernel(front, old_left, old_right, new_left, new_right, panels, pivots,
                 schur, panels_out, pivots_out,
                 tiles, results, lefts, rights, front_in, sides_in, rights_in, out,
                 panels_kept, pivots_kept, small_in, small_out):
    wide = front.shape[1] // TILES

    def near(ref, j):
        return ref.at[pl.ds(j * wide, wide)]

    sides = [
        pltpu.make_async_copy(source, lefts.at[n], sides_in.at[n])
        for n, source in enumerate((old_left, new_left))
    ]
    fetches = []
    for copy in sides:
        copy.start()
    for j in range(TILES):
        across = pl.ds(j * wide, wide)
        group = [
            pltpu.make_async_copy(near(source, j), near(rights.at[n], j), rights_in.at[n, j])
            for n, source in enumerate((old_right, new_right))
        ]
        group.append(
            pltpu.make_async_copy(front.at[:, across], tiles.at[j], front_in.at[j])
        )
        for copy in group:
            copy.start()
        fetches.append(group)
    small = (
        (panels, panels_kept, panels_out),
        (pivots, pivots_kept, pivots_out),
    )
    arrivals = [
        pltpu.make_async_copy(a, b, small_in.at[n]) for n, (a, b, _) in enumerate(small)
    ]
    leaving = [
        pltpu.make_async_copy(b, c, small_out.at[n]) for n, (_, b, c) in enumerate(small)
    ]
    for copy in arrivals:
        copy.start()
    for copy in sides:
        copy.wait()
    stores = []
    for j in range(TILES):
        for copy in fetches[j]:
            copy.wait()
        rows = slice(j * wide, (j + 1) * wide)
        update = times(lefts[0], rights[0, rows, :], NT) + times(lefts[1], rights[1, rows, :], NT)
        results[j] = tiles[j] - update
        store = pltpu.make_async_copy(
            results.at[j], schur.at[:, pl.ds(j * wide, wide)], out.at[j]
        )
        store.start()
        stores.append(store)
        if j == 0:
            for copy, onward in zip(arrivals, leaving):
                copy.wait()
                onward.start()
    for store in stores + leaving:
        store.wait()


TILES = 4


def body(front, prev_lower, prev_pivots, pivot_order):
    row_count, col_count = front.shape
    width = prev_lower.shape[1]
    vmem = pl.BlockSpec(memory_space=pltpu.VMEM)
    anywhere = pl.BlockSpec(memory_space=pl.ANY)
    shape = jax.ShapeDtypeStruct
    dma = pltpu.SemaphoreType.DMA
    scratch = pltpu.VMEM
    old_left, old_right, new_left, new_right, panels, pivots = pl.pallas_call(
        window_kernel,
        out_shape=[
            shape((row_count, width), BF16),
            shape((col_count, width), BF16),
            shape((row_count, width), BF16),
            shape((col_count, width), BF16),
            shape((CHUNK, 2 * width), F32),
            shape((1, 2 * width), F32),
        ],
        in_specs=[anywhere] * 4,
        out_specs=[anywhere] * 6,
        scratch_shapes=[
            scratch((CHUNK, width), BF16),
            scratch((1, width), F32),
            scratch(pivot_order.shape, jnp.int32),
            scratch((CHUNK, 2 * width), F32),
            scratch((1, 2 * width), F32),
            dma((3,)),
            scratch((row_count, width), BF16),
            scratch((row_count, width), BF16),
            scratch((col_count, width), BF16),
            scratch((row_count, width), BF16),
            scratch((row_count, width), BF16),
            scratch((col_count, width), BF16),
            scratch((CHUNK, width), BF16),
            scratch((CHUNK, width), BF16),
            scratch((2, 8, width), F32),
            scratch((row_count, width), BF16),
            scratch((row_count, width), BF16),
            scratch((2, 8, width), F32),
            scratch((width, width), F32),
            scratch((width, 2 * width), F32),
            scratch((row_count, 2 * width), F32),
            dma,
            dma((6,)),
            scratch((HALF, 2 * HALF), F32),
            scratch((2 * HALF, HALF), F32),
            scratch((2 * HALF, HALF), F32),
            scratch((2 * HALF, HALF), F32),
            scratch((8 * HALF, HALF), F32),
            scratch((320, HALF), F32),
            dma((4, 16)),
            dma((4,)),
        ]
        + Spread.semaphores() * 2
        + Corner.semaphores() * 2,
        compiler_params=pltpu.CompilerParams(
            collective_id=0, has_side_effects=True, vmem_limit_bytes=VMEM_LIMIT
        ),
        name="window",
    )(prev_lower, front, prev_pivots.reshape(1, width), pivot_order)
    tile = col_count // TILES
    schur, panels, pivots = pl.pallas_call(
        apply_kernel,
        out_shape=[
            shape((row_count, col_count), F32),
            shape((CHUNK, 2 * width), F32),
            shape((1, 2 * width), F32),
        ],
        in_specs=[anywhere] * 7,
        out_specs=[anywhere] * 3,
        scratch_shapes=[
            scratch((TILES, row_count, tile), F32),
            scratch((TILES, row_count, tile), F32),
            scratch((2, row_count, width), BF16),
            scratch((2, col_count, width), BF16),
            dma((TILES,)),
            dma((2,)),
            dma((2, TILES)),
            dma((TILES,)),
            scratch((CHUNK, 2 * width), F32),
            scratch((1, 2 * width), F32),
            dma((2,)),
            dma((2,)),
        ],
        compiler_params=pltpu.CompilerParams(vmem_limit_bytes=VMEM_LIMIT),
        name="apply",
    )(front, old_left, old_right, new_left, new_right, panels, pivots)
    return schur, panels, pivots.reshape(2 * width)


def solution(mesh):
    in_specs = (P(("grp", "row"), "col"), P(("grp", "row", "col"), None), P(), P())
    out_specs = (P(("grp", "row"), "col"), P(("grp", "row", "col"), None), P())
    return jax.shard_map(body, mesh=mesh, in_specs=in_specs, out_specs=out_specs, check_vma=False)
```

```python
import jax
import jax.numpy as jnp
from jax import lax
from jax.experimental import pallas as pl
from jax.experimental.pallas import tpu as pltpu
from jax.sharding import PartitionSpec as P

F32 = jnp.float32
BF16 = jnp.bfloat16
EXACT = lax.Precision.HIGHEST
MESH = pl.DeviceIdType.MESH
CHUNK = 32
WIDTH = 256
HALF = 128
TILES = 4
VMEM_LIMIT = 60 * 1024 * 1024


def place():
    return lax.axis_index("grp"), lax.axis_index("row"), lax.axis_index("col")


def remote(src, dst, send_sem, recv_sem, device):
    return pltpu.make_async_remote_copy(
        src_ref=src, dst_ref=dst, send_sem=send_sem, recv_sem=recv_sem,
        device_id=device, device_id_type=MESH,
    )


def signal(barrier, device):
    pl.semaphore_signal(barrier, inc=1, device_id=device, device_id_type=MESH)


def turn(value, step, size):
    return lax.rem(value + step + size, size)


def block(ref, number, rows):
    return ref.at[pl.ds(pl.multiple_of(number * rows, rows), rows)]


class Spread:
    def __init__(self, chunk, rows, cols, sems, full=None, lean=False):
        self.chunk, self.rows, self.cols, self.full = chunk, rows, cols, full
        self.lean = lean
        (self.zs, self.zr, self.fs, self.fr, self.ps, self.pr,
         self.xs, self.xr, self.cs, self.cr, self.own) = sems
        g, r, c = place()
        self.g, self.r, self.c = g, r, c
        self.x, self.yh, self.yl, self.z = r // 4, r % 4, c // 8, c % 8

    @staticmethod
    def semaphores():
        dma = pltpu.SemaphoreType.DMA
        return [dma, dma((7,)), dma, dma((8,)), dma((4,)), dma((4,)),
                dma, dma((3,)), dma, dma((4,)), dma((2,))]

    def target(self, j):
        return (self.r % 2, (self.c // 4) * 4 + j, self.g * 8 + self.r // 2)

    def source(self, i):
        return (self.c // 8, (2 * self.c + self.g) % 16, self.x * 4 + i)

    def is_me(self, device):
        return (device[0] == self.g) & (device[1] == self.r) & (device[2] == self.c)

    def greet(self, barrier):
        g, r, c = self.g, self.r, self.c
        for dz in range(1, 8):
            signal(barrier, (g, r, self.yl * 8 + turn(self.z, -dz, 8)))
        signal(barrier, (g, r, (1 - self.yl) * 8 + self.z))
        for dx in range(1, 4):
            signal(barrier, (g, turn(self.x, -dx, 4) * 4 + self.yh, c))
        signal(barrier, (1 - g, r, c))
        count = jnp.int32(12)
        for i in range(4):
            source = self.source(i)

            @pl.when(jnp.logical_not(self.is_me(source)))
            def _():
                signal(barrier, source)

            count += jnp.where(self.is_me(self.target(i)), 0, 1)
        return count

    def crossing(self, j):
        slot = (self.r % 2) * 16 + self.c
        return remote(self.chunk, block(self.cols, slot, CHUNK), self.ps.at[j],
                      self.pr.at[self.c % 4], self.target(j))

    def arriving(self, i):
        slot = self.g * 16 + self.x * 4 + i
        return remote(self.chunk, block(self.cols, slot, CHUNK), self.ps.at[i],
                      self.pr.at[i], self.source(i))

    def crossing_own(self):
        slot = (self.r % 2) * 16 + self.c
        return pltpu.make_async_copy(self.chunk, block(self.cols, slot, CHUNK), self.own.at[0])

    def across_z(self, dz, slot_z):
        return remote(self.chunk, block(self.rows, self.yl * 8 + slot_z, CHUNK),
                      self.zs, self.zr.at[dz - 1],
                      (self.g, self.r, self.yl * 8 + turn(self.z, dz, 8)))

    def partner(self, dz, side):
        slot = side * 8 + turn(self.z, -dz, 8)
        held = self.rows if self.full is None else self.full
        src = self.chunk if dz == 0 else block(held, slot, CHUNK)
        return remote(src, block(self.rows, slot, CHUNK), self.fs, self.fr.at[dz],
                      (self.g, self.r, (1 - self.yl) * 8 + self.z))

    def across_x(self, dx, x):
        part = block(self.cols, self.g * 4 + x, 4 * CHUNK)
        return remote(part, part, self.xs, self.xr.at[dx - 1],
                      (self.g, turn(self.x, dx, 4) * 4 + self.yh, self.c))

    def sibling(self, dx, grp):
        part = block(self.cols, grp * 4 + turn(self.x, -dx, 4), 4 * CHUNK)
        return remote(part, part, self.cs, self.cr.at[dx], (1 - self.g, self.r, self.c))

    def own_row_copy(self):
        return pltpu.make_async_copy(self.chunk, block(self.rows, self.c, CHUNK), self.own.at[1])

    def begin(self):
        for j in range(4):
            me = self.is_me(self.target(j))

            @pl.when(me)
            def _():
                self.crossing_own().start()

            @pl.when(jnp.logical_not(me))
            def _():
                self.crossing(j).start()

        for dz in range(1, 8):
            if self.lean:
                @pl.when((self.yl != 0) | (turn(self.z, dz, 8) != 0))
                def _():
                    self.across_z(dz, self.z).start()
            else:
                self.across_z(dz, self.z).start()
        for dz in range(1 if self.full is None else 8):
            self.pass_to_partner(dz)
        self.own_row_copy().start()

    def columns_arrive(self):
        for i in range(4):
            me = self.is_me(self.source(i))

            @pl.when(me)
            def _():
                self.crossing_own().wait()

            @pl.when(jnp.logical_not(me))
            def _():
                self.arriving(i).wait_recv()

    def columns_send(self):
        for dx in range(1, 4):
            self.across_x(dx, self.x).start()
        self.sibling(0, self.g).start()

    def urgent(self, grp, dx):
        return (grp == 0) & (turn(self.x, -dx, 4) < 2)

    def pass_rows(self):
        for dz in range(1, 8):
            self.across_z(dz, turn(self.z, -dz, 8)).wait_recv()
            self.pass_to_partner(dz)

    def pass_to_partner(self, dz):
        if self.lean:
            @pl.when(self.c != 8)
            def _():
                self.partner(dz, self.yl).start()
        else:
            self.partner(dz, self.yl).start()

    def pass_column(self, dx):
        self.across_x(dx, turn(self.x, -dx, 4)).wait_recv()
        self.sibling(dx, self.g).start()

    def pass_columns(self):
        for dx in range(1, 4):
            self.pass_column(dx)

    def finish_rows(self):
        self.own_row_copy().wait()
        for dz in range(8):
            self.partner(dz, 1 - self.yl).wait_recv()

    def finish_column(self, dx):
        self.sibling(dx, 1 - self.g).wait_recv()

    def finish_columns(self):
        for dx in range(4):
            self.finish_column(dx)

    def sent(self, part, sem):
        remote(part, part, sem, self.own.at[0], (1 - self.g, self.r, self.c)).wait_send()

    def drain(self):
        for j in range(4):
            @pl.when(jnp.logical_not(self.is_me(self.target(j))))
            def _():
                self.crossing(j).wait_send()

        if not self.lean:
            self.sent(self.rows.at[0:7 * CHUNK], self.zs)
            self.sent(self.rows.at[0:8 * CHUNK], self.fs)
            return

        @pl.when((self.yl == 0) & (self.z != 0))
        def _():
            self.sent(self.rows.at[0:6 * CHUNK], self.zs)

        @pl.when((self.yl != 0) | (self.z == 0))
        def _():
            self.sent(self.rows.at[0:7 * CHUNK], self.zs)

        @pl.when(self.c != 8)
        def _():
            self.sent(self.rows.at[0:8 * CHUNK], self.fs)

    def drain_columns(self):
        self.sent(self.cols.at[0:12 * CHUNK], self.xs)
        self.sent(self.cols.at[0:16 * CHUNK], self.cs)


class Corner:
    def __init__(self, front, first, corner, sems):
        self.front, self.first, self.corner = front, first, corner
        self.ts, self.tr, self.ys, self.yr, self.xs, self.xr, self.cs, self.cr = sems
        self.g, self.r, self.c = place()
        self.x, self.yh = self.r // 4, self.r % 4
        self.q = self.g * 16 + self.r
        self.rows = corner.shape[0] // 32
        self.lanes = corner.shape[1]

    @staticmethod
    def semaphores():
        dma = pltpu.SemaphoreType.DMA
        return [dma, dma, dma, dma((3,)), dma, dma((3,)), dma, dma((4,))]

    def greet(self, barrier):
        @pl.when(self.c == 0)
        def _():
            for dy in range(1, 4):
                signal(barrier, (self.g, self.x * 4 + turn(self.yh, -dy, 4), self.c))

            @pl.when(self.q != 0)
            def _():
                signal(barrier, (0, 0, 0))

        return jnp.where(self.c == 0, 3, 0) + jnp.where((self.q == 0) & (self.c == 0), 31, 0)

    def piece(self, slot):
        start = pl.multiple_of(self.first + slot * self.rows, self.rows)
        return self.front.at[pl.ds(start, self.rows), pl.ds(0, self.lanes)]

    def handing(self, slot):
        return remote(self.piece(slot), block(self.corner, slot, self.rows), self.ts,
                      self.tr, (slot // 16, slot % 16, 0))

    def keeping(self):
        return pltpu.make_async_copy(self.piece(0), block(self.corner, 0, self.rows), self.tr)

    def across_y(self, dy, yh):
        part = block(self.corner, self.g * 16 + self.x * 4 + yh, self.rows)
        return remote(part, part, self.ys, self.yr.at[dy - 1],
                      (self.g, self.x * 4 + turn(self.yh, dy, 4), self.c))

    def across_x(self, dx, x):
        part = block(self.corner, self.g * 4 + x, 4 * self.rows)
        return remote(part, part, self.xs, self.xr.at[dx - 1],
                      (self.g, turn(self.x, dx, 4) * 4 + self.yh, self.c))

    def sibling(self, dx, grp):
        part = block(self.corner, grp * 4 + turn(self.x, -dx, 4), 4 * self.rows)
        return remote(part, part, self.cs, self.cr.at[dx], (1 - self.g, self.r, self.c))

    def begin(self):
        @pl.when((self.q == 0) & (self.c == 0))
        def _():
            self.keeping().start()

            @pl.loop(1, 32)
            def _(slot):
                self.handing(slot).start()

    def first_hop(self):
        @pl.when(self.q == 0)
        def _():
            self.keeping().wait()

        @pl.when(self.q != 0)
        def _():
            self.handing(self.q).wait_recv()

        for dy in range(1, 4):
            self.across_y(dy, self.yh).start()

    def second_hop(self):
        for dy in range(1, 4):
            self.across_y(dy, turn(self.yh, -dy, 4)).wait_recv()
        for dx in range(1, 4):
            self.across_x(dx, self.x).start()
        self.sibling(0, self.g).start()

    def third_hop(self):
        for dx in range(1, 4):
            self.across_x(dx, turn(self.x, -dx, 4)).wait_recv()
            self.sibling(dx, self.g).start()

    def finish(self):
        for dx in range(4):
            self.sibling(dx, 1 - self.g).wait_recv()

    def drain(self):
        @pl.when(self.q == 0)
        def _():
            rest = pl.ds(self.rows, 31 * self.rows)
            start = pl.multiple_of(self.first + self.rows, self.rows)
            source = self.front.at[pl.ds(start, 31 * self.rows), pl.ds(0, self.lanes)]
            remote(source, self.corner.at[rest], self.ts, self.tr, (1, 0, 0)).wait_send()

        for part, sem in ((3, self.ys), (12, self.xs), (16, self.cs)):
            held = self.corner.at[pl.ds(0, part * self.rows)]
            remote(held, held, sem, self.tr, (1 - self.g, self.r, self.c)).wait_send()


def times(a, b, dims, precision=None):
    return lax.dot_general(
        a, b, (dims, ((), ())), precision=precision, preferred_element_type=F32
    )


NN = ((1,), (0,))
NT = ((1,), (1,))
TN = ((0,), (0,))


def inverted(value):
    guess = pl.reciprocal(value, approx=True)
    return guess * (2.0 - value * guess)


def panel_rows(value, row):
    ids = lax.broadcasted_iota(jnp.int32, (8, HALF), 0)
    multiplier = {}
    turned = {}
    kept = [None, None, None]

    def keep(k, items):
        for n, item in enumerate(items):
            kept[n] = item if kept[n] is None else jnp.where(ids == k, item, kept[n])

    for k in range(0, 8, 2):
        m = k + 1
        a, b, c = value[k, k], value[m, k], value[m, m]
        scale = inverted(a * c - b * b)
        for j in range(k + 2, 8):
            x, y = value[j, k], value[j, m]
            multiplier[j, k] = (c * x - b * y) * scale
            multiplier[j, m] = (a * y - b * x) * scale
        for j in range(k + 2, 8):
            for i in range(j, 8):
                value[i, j] = value[i, j] - (
                    multiplier[j, k] * value[i, k] + multiplier[j, m] * value[i, m]
                )
            for part in range(2):
                row[j][part] = row[j][part] - (
                    multiplier[j, k] * row[k][part] + multiplier[j, m] * row[m][part]
                )
        for part in range(2):
            x, y = row[k][part], row[m][part]
            turned[k, part] = (c * x - b * y) * scale
            turned[m, part] = (a * y - b * x) * scale
        first = inverted(a)
        ratio = b * first
        second = c - b * ratio
        keep(k, (row[k][1], a, first))
        keep(m, (row[m][1] - ratio * row[k][1], second, inverted(second)))
    for k in range(6, -1, -2):
        for m in (k, k + 1):
            for part in range(2):
                total = turned[m, part]
                for j in range(7, k + 1, -1):
                    total = total - multiplier[j, m] * turned[j, part]
                turned[m, part] = total
    return kept, turned


def eliminate(work, inverse, pivots, recips, columns, small, between=None):
    parts = (slice(0, HALF), slice(HALF, 2 * HALF))

    def spread_lane(tile, lane):
        return jnp.broadcast_to(tile[:, lane:lane + 1], (8, HALF))

    for number in range(16):
        if between is not None and number == 8:
            between()
        top = 8 * number
        mine = slice(top, top + 8)
        at = 64 * (number % 2)
        head = work[mine, parts[0]]
        for k in range(8):
            small[at + 8 * k:at + 8 * k + 8, :] = spread_lane(head, top + k)
        for i in range(number + 1, 16):
            tile = work[8 * i:8 * i + 8, parts[0]]
            if i == number + 1:
                soon = [spread_lane(tile, top + k) for k in range(8)]
                continue
            for k in range(8):
                columns[8 * (8 * i + k):8 * (8 * i + k) + 8, :] = spread_lane(tile, top + k)
        value = {
            (j, k): jnp.broadcast_to(
                small[at + 8 * k + j:at + 8 * k + j + 1, :], (8, HALF)
            )
            for k in range(8) for j in range(k, 8)
        }
        row = [
            [jnp.broadcast_to(work[top + k:top + k + 1, part], (8, HALF)) for part in parts]
            for k in range(8)
        ]
        kept, turned = panel_rows(value, row)
        inverse[mine, :] = kept[0]
        pivots[mine, :] = kept[1]
        recips[mine, :] = kept[2]
        for i in range(number + 1, 16):
            rows = slice(8 * i, 8 * i + 8)
            for part in range(2):
                terms = [
                    (soon[k] if i == number + 1 else
                     columns[8 * (8 * i + k):8 * (8 * i + k) + 8, :]) * turned[k, part]
                    for k in range(8)
                ]
                while len(terms) > 1:
                    terms = [x + y for x, y in zip(terms[::2], terms[1::2])]
                work[rows, parts[part]] = work[rows, parts[part]] - terms[0]


def factor(square, order, hooks, work, inverse, pivots, recips, columns, small):
    size = square.shape[0]
    ids = lax.broadcasted_iota(jnp.int32, (size, size), 0)
    chosen = (ids == order).astype(F32)
    moved = times(chosen, times(square, chosen, NN, EXACT), TN, EXACT)
    eye = (
        lax.broadcasted_iota(jnp.int32, (HALF, HALF), 0)
        == lax.broadcasted_iota(jnp.int32, (HALF, HALF), 1)
    ).astype(F32)
    lo, hi = slice(0, HALF), slice(HALF, 2 * HALF)
    work[:, lo] = moved[lo, lo]
    work[:, hi] = eye
    eliminate(work, inverse.at[lo], pivots.at[lo], recips.at[lo], columns, small)
    hooks[0]()
    first = inverse[lo, :]
    upper = times(first, moved[lo, hi], NN, EXACT)
    scaled = upper * recips[lo, :]
    work[:, lo] = moved[hi, hi] - times(scaled, upper, TN, EXACT)
    work[:, hi] = eye
    below = times(scaled, first, TN, EXACT)
    eliminate(work, inverse.at[hi], pivots.at[hi], recips.at[hi], columns, small, hooks[1])
    hooks[2]()
    second = inverse[hi, :]
    cross = -times(second, below, NN, EXACT)
    top = jnp.concatenate([first * recips[lo, :], jnp.zeros((HALF, HALF), F32)], axis=1)
    low = jnp.concatenate([cross * recips[hi, :], second * recips[hi, :]], axis=1)
    solver = times(jnp.concatenate([top, low], axis=0), chosen, NT, EXACT)
    values = jnp.concatenate([pivots[lo, :].T[0:1, :], pivots[hi, :].T[0:1, :]], axis=1)
    return solver, values


def nothing():
    pass


def window_kernel(
    chunk_in, whole, pivots_in, orders_in,
    updated_out, new_left_out, new_right_out, panels_out, pivots_out,
    prev_chunk, prev_pivots, orders, panels, pivots_kept, given_in, rows, rows_scaled, cols, new_rows, new_left, new_cols, chunk, second, shared,
    left, right, values, corner, edges, front, landed, kept, stored,
    work, inverse, pivots, recips, columns, small,
    send, recv, *sems,
):
    g, r, c = place()
    q = g * 16 + r
    split = len(Spread.semaphores())
    deal = len(Corner.semaphores())
    old = Spread(prev_chunk, rows, cols, sems[:split])
    top_square = Corner(whole, 0, corner, sems[2 * split:2 * split + deal])
    low_square = Corner(whole, WIDTH, edges, sems[2 * split + deal:])
    scratch = (work, inverse, pivots, recips, columns, small)
    lo, hi = slice(0, WIDTH), slice(WIDTH, 2 * WIDTH)
    inputs = [
        pltpu.make_async_copy(source, target, given_in.at[n])
        for n, (source, target) in enumerate(
            ((chunk_in, prev_chunk), (pivots_in, prev_pivots), (orders_in, orders))
        )
    ]
    for copy in inputs:
        copy.start()

    def handed(number, panel, to):
        device = (g, r, to)
        if number == 0:
            source, landing = block((left, right)[panel], to, CHUNK), (chunk, second)[panel]
        else:
            source = values.at[panel, pl.ds(pl.multiple_of(to * 8, 8), 8)]
            landing = shared.at[panel]
        return remote(source, landing, send.at[2 * number + panel],
                      recv.at[2 * number + panel], device)

    def keep_old():
        rows_scaled[...] = (rows[...].astype(F32) * before).astype(BF16)

    wide = front.shape[1] // TILES
    keeping = [
        pltpu.make_async_copy(
            front.at[:, pl.ds(j * wide, wide)], updated_out.at[:, pl.ds(j * wide, wide)],
            kept.at[j],
        )
        for j in range(TILES)
    ]

    def apply_old():
        for j in range(TILES):
            at = slice(j * wide, (j + 1) * wide)
            front[:, at] = front[:, at] - times(rows_scaled[...], cols[at, :], NT)
            keeping[j].start()

    keep_left = pltpu.make_async_copy(new_left, new_left_out, stored.at[2])
    keep_panels = pltpu.make_async_copy(panels, panels_out, stored.at[4])
    keep_pivots = pltpu.make_async_copy(pivots_kept, pivots_out, stored.at[5])
    keep_right = pltpu.make_async_copy(new_cols, new_right_out, stored.at[3])
    keep_near, keep_far = (
        pltpu.make_async_copy(
            new_cols.at[pl.ds(n * 2 * WIDTH, 2 * WIDTH)],
            new_right_out.at[pl.ds(n * 2 * WIDTH, 2 * WIDTH)], stored.at[n],
        )
        for n in range(2)
    )
    barrier = pltpu.get_barrier_semaphore()
    count = old.greet(barrier) + top_square.greet(barrier)

    @pl.when(c != 0)
    def _():
        signal(barrier, (g, r, 0))

    with jax.named_scope("barrier"):
        pl.semaphore_wait(barrier, count + jnp.where(c == 0, 15, 0))
    for copy in inputs:
        copy.wait()
    before = prev_pivots[...]
    top_square.begin()
    old.begin()
    low_square.begin()
    fetch = pltpu.make_async_copy(whole, front, landed)
    fetch.start()

    @pl.when(c == 0)
    def _():
        new = Spread(block(left, 0, CHUNK), new_rows, new_cols, sems[split:2 * split], left, True)
        with jax.named_scope("top_first"):
            top_square.first_hop()
        with jax.named_scope("columns_arrive"):
            old.columns_arrive()

        @pl.when(old.urgent(g, 0))
        def _():
            old.columns_send()

        with jax.named_scope("top_second"):
            top_square.second_hop()
        with jax.named_scope("columns_pass"):
            for dx in range(1, 4):
                @pl.when(old.urgent(g, dx))
                def _():
                    old.pass_column(dx)

        with jax.named_scope("top_third"):
            top_square.third_hop()
        with jax.named_scope("columns_finish"):
            for dx in range(4):
                @pl.when(old.urgent(1 - g, dx))
                def _():
                    old.finish_column(dx)

        @pl.when(jnp.logical_not(old.urgent(g, 0)))
        def _():
            old.columns_send()

        with jax.named_scope("low_first"):
            low_square.first_hop()
        near = cols[lo, :]
        near_scaled = (near.astype(F32) * before).astype(BF16)
        both = times(near_scaled, near, NT) + times(near, near_scaled, NT)
        with jax.named_scope("top_finish"):
            top_square.finish()

        def middle():
            with jax.named_scope("hook0"):
                low_square.second_hop()
                old.pass_rows()

        def late():
            with jax.named_scope("hook1"):
                for dx in range(1, 4):
                    @pl.when(jnp.logical_not(old.urgent(g, dx)))
                    def _():
                        old.pass_column(dx)

        def last():
            with jax.named_scope("hook2"):
                low_square.third_hop()

        with jax.named_scope("factor0"):
            solver, given = factor(
                corner[...] - 0.5 * both, orders[0:1, :], (middle, late, nothing), *scratch
            )
        values[0] = jnp.broadcast_to(given, (128, WIDTH))
        last()
        with jax.named_scope("wait_rows"):
            fetch.wait()
            old.finish_rows()
        with jax.named_scope("panel0"):
            keep_old()
            panel = front[:, lo] - times(rows_scaled[...], near, NT)
            shown = times(panel, solver, NT, EXACT).astype(BF16)
            left[...] = shown
        with jax.named_scope("wait_low"):
            for dx in range(4):
                @pl.when(jnp.logical_not(old.urgent(1 - g, dx)))
                def _():
                    old.finish_column(dx)

            low_square.finish()
        with jax.named_scope("edge"):
            next_near = cols[hi, :]
            next_scaled = (next_near.astype(F32) * before).astype(BF16)
            edge = edges[:, lo] - times(next_scaled, near, NT)
            edge = times(edge, solver, NT, EXACT).astype(BF16)
        with jax.named_scope("scatter"):
            for to in range(1, 16):
                handed(0, 0, to).start()
            new.begin()
            for to in range(1, 16):
                handed(1, 0, to).start()
        edge_scaled = (edge.astype(F32) * given).astype(BF16)
        both = times(next_scaled, next_near, NT) + times(next_near, next_scaled, NT)
        more = times(edge_scaled, edge, NT) + times(edge, edge_scaled, NT)
        square = (edges[:, hi] - 0.5 * both) - 0.5 * more

        with jax.named_scope("factor1"):
            solver, later = factor(
                square, orders[1:2, :], (nothing, nothing, nothing), *scratch
            )
        values[1] = jnp.broadcast_to(later, (128, WIDTH))
        with jax.named_scope("panel1"):
            shown_scaled = (left[...].astype(F32) * given).astype(BF16)
            panel = front[:, hi] - times(rows_scaled[...], next_near, NT)
            panel = panel - times(shown_scaled, edge, NT)
            right[...] = times(panel, solver, NT, EXACT).astype(BF16)
        @pl.when(q != 0)
        def _():
            new_left[...] = shown_scaled

        @pl.when(q == 0)
        def _():
            new_left[lo, :] = jnp.zeros_like(new_left[lo, :])
            new_left[hi, :] = shown_scaled[hi]

        chunk[...] = left[0:CHUNK, :]
        shared[...] = values[:, 0:8, :]
        for to in range(1, 16):
            handed(1, 1, to).start()
            handed(0, 1, to).start()
        second[...] = right[0:CHUNK, :]
        with jax.named_scope("apply_old"):
            apply_old()
        with jax.named_scope("arrive"):
            new.columns_arrive()

        @pl.when(g == 1)
        def _():
            new.columns_send()

        new_cols[lo, :] = jnp.zeros((WIDTH, WIDTH), BF16)
        new_cols[hi, :] = edge
        keep_near.start()
        keep_left.start()
        with jax.named_scope("last_columns"):
            @pl.when(g == 1)
            def _():
                new.pass_columns()

            @pl.when(g == 0)
            def _():
                new.finish_columns()

        keep_far.start()

    @pl.when(c != 0)
    def _():
        with jax.named_scope("old"):
            old.pass_rows()
            old.columns_arrive()
            old.columns_send()
            old.pass_columns()
            old.finish_rows()
            old.finish_columns()
        keep_old()
        fetch.wait()
        apply_old()
        new = Spread(chunk, new_rows, new_cols, sems[split:2 * split], None, True)
        with jax.named_scope("recv_chunk"):
            handed(0, 0, c).wait_recv()
        new.begin()
        with jax.named_scope("pass_rows"):
            new.pass_rows()
        with jax.named_scope("columns_arrive"):
            new.columns_arrive()
            new.columns_send()
        with jax.named_scope("pass_columns"):
            new.pass_columns()
        with jax.named_scope("finish_rows"):
            new.finish_rows()
            handed(1, 0, c).wait_recv()
        given = shared[0, 0:1, :]

        @pl.when(q != 0)
        def _():
            new_left[...] = (new_rows[...].astype(F32) * given).astype(BF16)

        @pl.when(q == 0)
        def _():
            new_left[lo, :] = jnp.zeros_like(new_left[lo, :])
            new_left[hi, :] = (new_rows[hi, :].astype(F32) * given).astype(BF16)

        keep_left.start()
        with jax.named_scope("finish_columns"):
            new.finish_columns()
        keep_right.start()
        with jax.named_scope("recv_values"):
            handed(1, 1, c).wait_recv()
            handed(0, 1, c).wait_recv()
        new.drain()
        new.drain_columns()

    given, later = shared[0, 0:1, :], shared[1, 0:1, :]
    panels[:, lo] = chunk[...].astype(F32) * given
    live = (q != 0) | (c >= WIDTH // CHUNK)

    @pl.when(live)
    def _():
        panels[:, hi] = second[...].astype(F32) * later

    @pl.when(jnp.logical_not(live))
    def _():
        panels[:, hi] = jnp.zeros((CHUNK, WIDTH), F32)

    pivots_kept[:, lo] = given
    pivots_kept[:, hi] = later
    keep_panels.start()
    keep_pivots.start()
    @pl.when(c == 0)
    def _():
        new = Spread(block(left, 0, CHUNK), new_rows, new_cols, sems[split:2 * split], left, True)
        with jax.named_scope("drain_last"):
            new.own_row_copy().wait()
            new.drain()

            @pl.when(g == 1)
            def _():
                new.drain_columns()

            for panel in range(2):
                rest = (left, right)[panel].at[CHUNK:16 * CHUNK]
                remote(rest, rest, send.at[panel], recv.at[panel], (1 - g, r, c)).wait_send()
                rest = values.at[panel, 8:128]
                remote(rest, rest, send.at[2 + panel], recv.at[2 + panel], (1 - g, r, c)).wait_send()
            top_square.drain()
            low_square.drain()
            keep_near.wait()
            keep_far.wait()

    @pl.when(c != 0)
    def _():
        keep_right.wait()

    with jax.named_scope("drain_old"):
        old.drain()
        old.drain_columns()
        for copy in (*keeping, keep_left, keep_panels, keep_pivots):
            copy.wait()


def apply_kernel(front, new_left, new_right, panels, pivots,
                 schur, panels_out, pivots_out,
                 tiles, results, left, right, front_in, left_in, right_in, out,
                 panels_kept, pivots_kept, small_in, small_out):
    wide = front.shape[1] // TILES
    side = pltpu.make_async_copy(new_left, left, left_in)
    side.start()
    fetches = []
    for j in range(TILES):
        at = pl.ds(j * wide, wide)
        group = (
            pltpu.make_async_copy(new_right.at[at], right.at[at], right_in.at[j]),
            pltpu.make_async_copy(front.at[:, at], tiles.at[j], front_in.at[j]),
        )
        for copy in group:
            copy.start()
        fetches.append(group)
    small = (
        (panels, panels_kept, panels_out),
        (pivots, pivots_kept, pivots_out),
    )
    arrivals = [
        pltpu.make_async_copy(a, b, small_in.at[n]) for n, (a, b, _) in enumerate(small)
    ]
    leaving = [
        pltpu.make_async_copy(b, c, small_out.at[n]) for n, (_, b, c) in enumerate(small)
    ]
    for copy in arrivals:
        copy.start()
    side.wait()
    stores = []
    for j in range(TILES):
        for copy in fetches[j]:
            copy.wait()
        rows = slice(j * wide, (j + 1) * wide)
        results[j] = tiles[j] - times(left[...], right[rows, :], NT)
        store = pltpu.make_async_copy(
            results.at[j], schur.at[:, pl.ds(j * wide, wide)], out.at[j]
        )
        store.start()
        stores.append(store)
        if j == 0:
            for copy, onward in zip(arrivals, leaving):
                copy.wait()
                onward.start()
    for store in stores + leaving:
        store.wait()


def body(front, prev_lower, prev_pivots, pivot_order):
    row_count, col_count = front.shape
    width = prev_lower.shape[1]
    vmem = pl.BlockSpec(memory_space=pltpu.VMEM)
    anywhere = pl.BlockSpec(memory_space=pl.ANY)
    shape = jax.ShapeDtypeStruct
    dma = pltpu.SemaphoreType.DMA
    scratch = pltpu.VMEM
    updated, new_left, new_right, panels, pivots = pl.pallas_call(
        window_kernel,
        out_shape=[
            shape((row_count, col_count), F32),
            shape((row_count, width), BF16),
            shape((col_count, width), BF16),
            shape((CHUNK, 2 * width), F32),
            shape((1, 2 * width), F32),
        ],
        in_specs=[anywhere] * 4,
        out_specs=[anywhere] * 5,
        scratch_shapes=[
            scratch((CHUNK, width), BF16),
            scratch((1, width), F32),
            scratch(pivot_order.shape, jnp.int32),
            scratch((CHUNK, 2 * width), F32),
            scratch((1, 2 * width), F32),
            dma((3,)),
            scratch((row_count, width), BF16),
            scratch((row_count, width), BF16),
            scratch((col_count, width), BF16),
            scratch((row_count, width), BF16),
            scratch((row_count, width), BF16),
            scratch((col_count, width), BF16),
            scratch((CHUNK, width), BF16),
            scratch((CHUNK, width), BF16),
            scratch((2, 8, width), F32),
            scratch((row_count, width), BF16),
            scratch((row_count, width), BF16),
            scratch((2, 128, width), F32),
            scratch((width, width), F32),
            scratch((width, 2 * width), F32),
            scratch((row_count, col_count), F32),
            dma,
            dma((TILES,)),
            dma((6,)),
            scratch((HALF, 2 * HALF), F32),
            scratch((2 * HALF, HALF), F32),
            scratch((2 * HALF, HALF), F32),
            scratch((2 * HALF, HALF), F32),
            scratch((8 * HALF, HALF), F32),
            scratch((HALF, HALF), F32),
            dma((4,)),
            dma((4,)),
        ]
        + Spread.semaphores() * 2
        + Corner.semaphores() * 2,
        compiler_params=pltpu.CompilerParams(
            collective_id=0, has_side_effects=True, vmem_limit_bytes=VMEM_LIMIT
        ),
        name="window",
    )(prev_lower, front, prev_pivots.reshape(1, width), pivot_order)
    tile = col_count // TILES
    schur, panels, pivots = pl.pallas_call(
        apply_kernel,
        out_shape=[
            shape((row_count, col_count), F32),
            shape((CHUNK, 2 * width), F32),
            shape((1, 2 * width), F32),
        ],
        in_specs=[anywhere] * 5,
        out_specs=[anywhere] * 3,
        scratch_shapes=[
            scratch((TILES, row_count, tile), F32),
            scratch((TILES, row_count, tile), F32),
            scratch((row_count, width), BF16),
            scratch((col_count, width), BF16),
            dma((TILES,)),
            dma,
            dma((TILES,)),
            dma((TILES,)),
            scratch((CHUNK, 2 * width), F32),
            scratch((1, 2 * width), F32),
            dma((2,)),
            dma((2,)),
        ],
        compiler_params=pltpu.CompilerParams(vmem_limit_bytes=VMEM_LIMIT),
        name="apply",
    )(updated, new_left, new_right, panels, pivots)
    return schur, panels, pivots.reshape(2 * width)


def solution(mesh):
    in_specs = (P(("grp", "row"), "col"), P(("grp", "row", "col"), None), P(), P())
    out_specs = (P(("grp", "row"), "col"), P(("grp", "row", "col"), None), P())
    return jax.shard_map(body, mesh=mesh, in_specs=in_specs, out_specs=out_specs, check_vma=False)
```

```python
import jax
import jax.numpy as jnp
from jax import lax
from jax.experimental import pallas as pl
from jax.experimental.pallas import tpu as pltpu
from jax.sharding import PartitionSpec as P

F32 = jnp.float32
BF16 = jnp.bfloat16
EXACT = lax.Precision.HIGHEST
MESH = pl.DeviceIdType.MESH
CHUNK = 32
WIDTH = 256
HALF = 128
TILES = 4
VMEM_LIMIT = 60 * 1024 * 1024


def place():
    return lax.axis_index("grp"), lax.axis_index("row"), lax.axis_index("col")


def remote(src, dst, send_sem, recv_sem, device):
    return pltpu.make_async_remote_copy(
        src_ref=src, dst_ref=dst, send_sem=send_sem, recv_sem=recv_sem,
        device_id=device, device_id_type=MESH,
    )


def signal(barrier, device):
    pl.semaphore_signal(barrier, inc=1, device_id=device, device_id_type=MESH)


def turn(value, step, size):
    return lax.rem(value + step + size, size)


def block(ref, number, rows):
    return ref.at[pl.ds(pl.multiple_of(number * rows, rows), rows)]


class Spread:
    def __init__(self, chunk, rows, cols, sems, full=None, lean=False):
        self.chunk, self.rows, self.cols, self.full = chunk, rows, cols, full
        self.lean = lean
        (self.zs, self.zr, self.fs, self.fr, self.ps, self.pr,
         self.xs, self.xr, self.cs, self.cr, self.own) = sems
        g, r, c = place()
        self.g, self.r, self.c = g, r, c
        self.x, self.yh, self.yl, self.z = r // 4, r % 4, c // 8, c % 8

    @staticmethod
    def semaphores():
        dma = pltpu.SemaphoreType.DMA
        return [dma, dma((7,)), dma, dma((8,)), dma((4,)), dma((4,)),
                dma, dma((3,)), dma, dma((4,)), dma((2,))]

    def target(self, j):
        return (self.r % 2, (self.c // 4) * 4 + j, self.g * 8 + self.r // 2)

    def source(self, i):
        return (self.c // 8, (2 * self.c + self.g) % 16, self.x * 4 + i)

    def is_me(self, device):
        return (device[0] == self.g) & (device[1] == self.r) & (device[2] == self.c)

    def greet(self, barrier):
        g, r, c = self.g, self.r, self.c
        for dz in range(1, 8):
            signal(barrier, (g, r, self.yl * 8 + turn(self.z, -dz, 8)))
        signal(barrier, (g, r, (1 - self.yl) * 8 + self.z))
        for dx in range(1, 4):
            signal(barrier, (g, turn(self.x, -dx, 4) * 4 + self.yh, c))
        signal(barrier, (1 - g, r, c))
        count = jnp.int32(12)
        for i in range(4):
            source = self.source(i)

            @pl.when(jnp.logical_not(self.is_me(source)))
            def _():
                signal(barrier, source)

            count += jnp.where(self.is_me(self.target(i)), 0, 1)
        return count

    def crossing(self, j):
        slot = (self.r % 2) * 16 + self.c
        return remote(self.chunk, block(self.cols, slot, CHUNK), self.ps.at[j],
                      self.pr.at[self.c % 4], self.target(j))

    def arriving(self, i):
        slot = self.g * 16 + self.x * 4 + i
        return remote(self.chunk, block(self.cols, slot, CHUNK), self.ps.at[i],
                      self.pr.at[i], self.source(i))

    def crossing_own(self):
        slot = (self.r % 2) * 16 + self.c
        return pltpu.make_async_copy(self.chunk, block(self.cols, slot, CHUNK), self.own.at[0])

    def across_z(self, dz, slot_z):
        return remote(self.chunk, block(self.rows, self.yl * 8 + slot_z, CHUNK),
                      self.zs, self.zr.at[dz - 1],
                      (self.g, self.r, self.yl * 8 + turn(self.z, dz, 8)))

    def partner(self, dz, side):
        slot = side * 8 + turn(self.z, -dz, 8)
        held = self.rows if self.full is None else self.full
        src = self.chunk if dz == 0 else block(held, slot, CHUNK)
        return remote(src, block(self.rows, slot, CHUNK), self.fs, self.fr.at[dz],
                      (self.g, self.r, (1 - self.yl) * 8 + self.z))

    def across_x(self, dx, x):
        part = block(self.cols, self.g * 4 + x, 4 * CHUNK)
        return remote(part, part, self.xs, self.xr.at[dx - 1],
                      (self.g, turn(self.x, dx, 4) * 4 + self.yh, self.c))

    def sibling(self, dx, grp):
        part = block(self.cols, grp * 4 + turn(self.x, -dx, 4), 4 * CHUNK)
        return remote(part, part, self.cs, self.cr.at[dx], (1 - self.g, self.r, self.c))

    def own_row_copy(self):
        return pltpu.make_async_copy(self.chunk, block(self.rows, self.c, CHUNK), self.own.at[1])

    def begin(self):
        for j in range(4):
            me = self.is_me(self.target(j))

            @pl.when(me)
            def _():
                self.crossing_own().start()

            @pl.when(jnp.logical_not(me))
            def _():
                self.crossing(j).start()

        for dz in range(1, 8):
            if self.lean:
                @pl.when((self.yl != 0) | (turn(self.z, dz, 8) != 0))
                def _():
                    self.across_z(dz, self.z).start()
            else:
                self.across_z(dz, self.z).start()
        for dz in range(1 if self.full is None else 8):
            self.pass_to_partner(dz)
        self.own_row_copy().start()

    def columns_arrive(self):
        for i in range(4):
            me = self.is_me(self.source(i))

            @pl.when(me)
            def _():
                self.crossing_own().wait()

            @pl.when(jnp.logical_not(me))
            def _():
                self.arriving(i).wait_recv()

    def columns_send(self):
        for dx in range(1, 4):
            self.across_x(dx, self.x).start()
        self.sibling(0, self.g).start()

    def urgent(self, grp, dx):
        return (grp == 0) & (turn(self.x, -dx, 4) < 2)

    def pass_rows(self):
        for dz in range(1, 8):
            self.across_z(dz, turn(self.z, -dz, 8)).wait_recv()
            self.pass_to_partner(dz)

    def pass_to_partner(self, dz):
        if self.lean:
            @pl.when(self.c != 8)
            def _():
                self.partner(dz, self.yl).start()
        else:
            self.partner(dz, self.yl).start()

    def pass_column(self, dx):
        self.across_x(dx, turn(self.x, -dx, 4)).wait_recv()
        self.sibling(dx, self.g).start()

    def pass_columns(self):
        for dx in range(1, 4):
            self.pass_column(dx)

    def finish_rows(self):
        self.own_row_copy().wait()
        for dz in range(8):
            self.partner(dz, 1 - self.yl).wait_recv()

    def finish_column(self, dx):
        self.sibling(dx, 1 - self.g).wait_recv()

    def finish_columns(self):
        for dx in range(4):
            self.finish_column(dx)

    def sent(self, part, sem):
        remote(part, part, sem, self.own.at[0], (1 - self.g, self.r, self.c)).wait_send()

    def drain(self):
        for j in range(4):
            @pl.when(jnp.logical_not(self.is_me(self.target(j))))
            def _():
                self.crossing(j).wait_send()

        if not self.lean:
            self.sent(self.rows.at[0:7 * CHUNK], self.zs)
            self.sent(self.rows.at[0:8 * CHUNK], self.fs)
            return

        @pl.when((self.yl == 0) & (self.z != 0))
        def _():
            self.sent(self.rows.at[0:6 * CHUNK], self.zs)

        @pl.when((self.yl != 0) | (self.z == 0))
        def _():
            self.sent(self.rows.at[0:7 * CHUNK], self.zs)

        @pl.when(self.c != 8)
        def _():
            self.sent(self.rows.at[0:8 * CHUNK], self.fs)

    def drain_columns(self):
        self.sent(self.cols.at[0:12 * CHUNK], self.xs)
        self.sent(self.cols.at[0:16 * CHUNK], self.cs)


class Corner:
    def __init__(self, front, first, corner, sems):
        self.front, self.first, self.corner = front, first, corner
        self.ts, self.tr, self.ys, self.yr, self.xs, self.xr, self.cs, self.cr = sems
        self.g, self.r, self.c = place()
        self.x, self.yh = self.r // 4, self.r % 4
        self.q = self.g * 16 + self.r
        self.rows = corner.shape[0] // 32
        self.lanes = corner.shape[1]

    @staticmethod
    def semaphores():
        dma = pltpu.SemaphoreType.DMA
        return [dma, dma, dma, dma((3,)), dma, dma((3,)), dma, dma((4,))]

    def greet(self, barrier):
        @pl.when(self.c == 0)
        def _():
            for dy in range(1, 4):
                signal(barrier, (self.g, self.x * 4 + turn(self.yh, -dy, 4), self.c))

            @pl.when(self.q != 0)
            def _():
                signal(barrier, (0, 0, 0))

        return jnp.where(self.c == 0, 3, 0) + jnp.where((self.q == 0) & (self.c == 0), 31, 0)

    def piece(self, slot):
        start = pl.multiple_of(self.first + slot * self.rows, self.rows)
        return self.front.at[pl.ds(start, self.rows), pl.ds(0, self.lanes)]

    def handing(self, slot):
        return remote(self.piece(slot), block(self.corner, slot, self.rows), self.ts,
                      self.tr, (slot // 16, slot % 16, 0))

    def keeping(self):
        return pltpu.make_async_copy(self.piece(0), block(self.corner, 0, self.rows), self.tr)

    def across_y(self, dy, yh):
        part = block(self.corner, self.g * 16 + self.x * 4 + yh, self.rows)
        return remote(part, part, self.ys, self.yr.at[dy - 1],
                      (self.g, self.x * 4 + turn(self.yh, dy, 4), self.c))

    def across_x(self, dx, x):
        part = block(self.corner, self.g * 4 + x, 4 * self.rows)
        return remote(part, part, self.xs, self.xr.at[dx - 1],
                      (self.g, turn(self.x, dx, 4) * 4 + self.yh, self.c))

    def sibling(self, dx, grp):
        part = block(self.corner, grp * 4 + turn(self.x, -dx, 4), 4 * self.rows)
        return remote(part, part, self.cs, self.cr.at[dx], (1 - self.g, self.r, self.c))

    def begin(self):
        @pl.when((self.q == 0) & (self.c == 0))
        def _():
            self.keeping().start()

            @pl.loop(1, 32)
            def _(slot):
                self.handing(slot).start()

    def first_hop(self):
        @pl.when(self.q == 0)
        def _():
            self.keeping().wait()

        @pl.when(self.q != 0)
        def _():
            self.handing(self.q).wait_recv()

        for dy in range(1, 4):
            self.across_y(dy, self.yh).start()

    def second_hop(self):
        for dy in range(1, 4):
            self.across_y(dy, turn(self.yh, -dy, 4)).wait_recv()
        for dx in range(1, 4):
            self.across_x(dx, self.x).start()
        self.sibling(0, self.g).start()

    def third_hop(self):
        for dx in range(1, 4):
            self.across_x(dx, turn(self.x, -dx, 4)).wait_recv()
            self.sibling(dx, self.g).start()

    def finish(self):
        for dx in range(4):
            self.sibling(dx, 1 - self.g).wait_recv()

    def drain(self):
        @pl.when(self.q == 0)
        def _():
            rest = pl.ds(self.rows, 31 * self.rows)
            start = pl.multiple_of(self.first + self.rows, self.rows)
            source = self.front.at[pl.ds(start, 31 * self.rows), pl.ds(0, self.lanes)]
            remote(source, self.corner.at[rest], self.ts, self.tr, (1, 0, 0)).wait_send()

        for part, sem in ((3, self.ys), (12, self.xs), (16, self.cs)):
            held = self.corner.at[pl.ds(0, part * self.rows)]
            remote(held, held, sem, self.tr, (1 - self.g, self.r, self.c)).wait_send()


def times(a, b, dims, precision=None):
    return lax.dot_general(
        a, b, (dims, ((), ())), precision=precision, preferred_element_type=F32
    )


NN = ((1,), (0,))
NT = ((1,), (1,))
TN = ((0,), (0,))


def inverted(value):
    guess = pl.reciprocal(value, approx=True)
    return guess * (2.0 - value * guess)


def panel_rows(value, row):
    ids = lax.broadcasted_iota(jnp.int32, (8, HALF), 0)
    multiplier = {}
    turned = {}
    kept = [None, None, None]

    def keep(k, items):
        for n, item in enumerate(items):
            kept[n] = item if kept[n] is None else jnp.where(ids == k, item, kept[n])

    for k in range(0, 8, 2):
        m = k + 1
        a, b, c = value[k, k], value[m, k], value[m, m]
        scale = inverted(a * c - b * b)
        for j in range(k + 2, 8):
            x, y = value[j, k], value[j, m]
            multiplier[j, k] = (c * x - b * y) * scale
            multiplier[j, m] = (a * y - b * x) * scale
        for j in range(k + 2, 8):
            for i in range(j, 8):
                value[i, j] = value[i, j] - (
                    multiplier[j, k] * value[i, k] + multiplier[j, m] * value[i, m]
                )
            for part in range(2):
                row[j][part] = row[j][part] - (
                    multiplier[j, k] * row[k][part] + multiplier[j, m] * row[m][part]
                )
        for part in range(2):
            x, y = row[k][part], row[m][part]
            turned[k, part] = (c * x - b * y) * scale
            turned[m, part] = (a * y - b * x) * scale
        first = inverted(a)
        ratio = b * first
        second = c - b * ratio
        keep(k, (row[k][1], a, first))
        keep(m, (row[m][1] - ratio * row[k][1], second, inverted(second)))
    for k in range(6, -1, -2):
        for m in (k, k + 1):
            for part in range(2):
                total = turned[m, part]
                for j in range(7, k + 1, -1):
                    total = total - multiplier[j, m] * turned[j, part]
                turned[m, part] = total
    return kept, turned


def eliminate(work, inverse, pivots, recips, columns, small, between=None):
    parts = (slice(0, HALF), slice(HALF, 2 * HALF))

    def spread_lane(tile, lane):
        return jnp.broadcast_to(tile[:, lane:lane + 1], (8, HALF))

    for number in range(16):
        if between is not None and number == 8:
            between()
        top = 8 * number
        mine = slice(top, top + 8)
        at = 64 * (number % 2)
        head = work[mine, parts[0]]
        for k in range(8):
            small[at + 8 * k:at + 8 * k + 8, :] = spread_lane(head, top + k)
        for i in range(number + 1, 16):
            tile = work[8 * i:8 * i + 8, parts[0]]
            if i == number + 1:
                soon = [spread_lane(tile, top + k) for k in range(8)]
                continue
            for k in range(8):
                columns[8 * (8 * i + k):8 * (8 * i + k) + 8, :] = spread_lane(tile, top + k)
        value = {
            (j, k): jnp.broadcast_to(
                small[at + 8 * k + j:at + 8 * k + j + 1, :], (8, HALF)
            )
            for k in range(8) for j in range(k, 8)
        }
        row = [
            [jnp.broadcast_to(work[top + k:top + k + 1, part], (8, HALF)) for part in parts]
            for k in range(8)
        ]
        kept, turned = panel_rows(value, row)
        inverse[mine, :] = kept[0]
        pivots[mine, :] = kept[1]
        recips[mine, :] = kept[2]
        for i in range(number + 1, 16):
            rows = slice(8 * i, 8 * i + 8)
            for part in range(2):
                terms = [
                    (soon[k] if i == number + 1 else
                     columns[8 * (8 * i + k):8 * (8 * i + k) + 8, :]) * turned[k, part]
                    for k in range(8)
                ]
                while len(terms) > 1:
                    terms = [x + y for x, y in zip(terms[::2], terms[1::2])]
                work[rows, parts[part]] = work[rows, parts[part]] - terms[0]


def factor(square, order, hooks, work, inverse, pivots, recips, columns, small):
    size = square.shape[0]
    ids = lax.broadcasted_iota(jnp.int32, (size, size), 0)
    chosen = (ids == order).astype(F32)
    moved = times(chosen, times(square, chosen, NN, EXACT), TN, EXACT)
    eye = (
        lax.broadcasted_iota(jnp.int32, (HALF, HALF), 0)
        == lax.broadcasted_iota(jnp.int32, (HALF, HALF), 1)
    ).astype(F32)
    lo, hi = slice(0, HALF), slice(HALF, 2 * HALF)
    work[:, lo] = moved[lo, lo]
    work[:, hi] = eye
    eliminate(work, inverse.at[lo], pivots.at[lo], recips.at[lo], columns, small)
    hooks[0]()
    first = inverse[lo, :]
    upper = times(first, moved[lo, hi], NN, EXACT)
    scaled = upper * recips[lo, :]
    work[:, lo] = moved[hi, hi] - times(scaled, upper, TN, EXACT)
    work[:, hi] = eye
    below = times(scaled, first, TN, EXACT)
    eliminate(work, inverse.at[hi], pivots.at[hi], recips.at[hi], columns, small, hooks[1])
    hooks[2]()
    second = inverse[hi, :]
    cross = -times(second, below, NN, EXACT)
    top = jnp.concatenate([first * recips[lo, :], jnp.zeros((HALF, HALF), F32)], axis=1)
    low = jnp.concatenate([cross * recips[hi, :], second * recips[hi, :]], axis=1)
    solver = times(jnp.concatenate([top, low], axis=0), chosen, NT, EXACT)
    values = jnp.concatenate([pivots[lo, :].T[0:1, :], pivots[hi, :].T[0:1, :]], axis=1)
    return solver, values


def nothing():
    pass


def window_kernel(
    chunk_in, whole, pivots_in, orders_in,
    updated_out, new_left_out, new_right_out, panels_out, pivots_out,
    prev_chunk, prev_pivots, orders, panels, pivots_kept, given_in, rows, rows_scaled, cols, new_rows, new_left, new_cols, chunk, second, shared,
    left, right, values, corner, edges, front, landed, kept, stored,
    work, inverse, pivots, recips, columns, small,
    send, recv, *sems,
):
    g, r, c = place()
    q = g * 16 + r
    split = len(Spread.semaphores())
    deal = len(Corner.semaphores())
    old = Spread(prev_chunk, rows, cols, sems[:split])
    top_square = Corner(whole, 0, corner, sems[2 * split:2 * split + deal])
    low_square = Corner(whole, WIDTH, edges, sems[2 * split + deal:])
    scratch = (work, inverse, pivots, recips, columns, small)
    lo, hi = slice(0, WIDTH), slice(WIDTH, 2 * WIDTH)
    inputs = [
        pltpu.make_async_copy(source, target, given_in.at[n])
        for n, (source, target) in enumerate(
            ((chunk_in, prev_chunk), (pivots_in, prev_pivots), (orders_in, orders))
        )
    ]
    for copy in inputs:
        copy.start()

    def handed(number, panel, to):
        device = (g, r, to)
        if number == 0:
            source, landing = block((left, right)[panel], to, CHUNK), (chunk, second)[panel]
        else:
            source = values.at[panel, pl.ds(pl.multiple_of(to * 8, 8), 8)]
            landing = shared.at[panel]
        return remote(source, landing, send.at[2 * number + panel],
                      recv.at[2 * number + panel], device)

    def keep_old():
        rows_scaled[...] = (rows[...].astype(F32) * before).astype(BF16)

    wide = front.shape[1] // TILES
    keeping = [
        pltpu.make_async_copy(
            front.at[:, pl.ds(j * wide, wide)], updated_out.at[:, pl.ds(j * wide, wide)],
            kept.at[j],
        )
        for j in range(TILES)
    ]

    def apply_old():
        for j in range(TILES):
            at = slice(j * wide, (j + 1) * wide)
            front[:, at] = front[:, at] - times(rows_scaled[...], cols[at, :], NT)
            keeping[j].start()

    keep_left = pltpu.make_async_copy(new_left, new_left_out, stored.at[2])
    keep_panels = pltpu.make_async_copy(panels, panels_out, stored.at[4])
    keep_pivots = pltpu.make_async_copy(pivots_kept, pivots_out, stored.at[5])
    keep_right = pltpu.make_async_copy(new_cols, new_right_out, stored.at[3])
    keep_near, keep_far = (
        pltpu.make_async_copy(
            new_cols.at[pl.ds(n * 2 * WIDTH, 2 * WIDTH)],
            new_right_out.at[pl.ds(n * 2 * WIDTH, 2 * WIDTH)], stored.at[n],
        )
        for n in range(2)
    )
    barrier = pltpu.get_barrier_semaphore()
    count = old.greet(barrier) + top_square.greet(barrier)

    @pl.when(c != 0)
    def _():
        signal(barrier, (g, r, 0))

    with jax.named_scope("barrier"):
        pl.semaphore_wait(barrier, count + jnp.where(c == 0, 15, 0))
    for copy in inputs:
        copy.wait()
    before = prev_pivots[...]
    top_square.begin()
    old.begin()
    low_square.begin()
    fetch = pltpu.make_async_copy(whole, front, landed)
    fetch.start()

    @pl.when(c == 0)
    def _():
        new = Spread(block(left, 0, CHUNK), new_rows, new_cols, sems[split:2 * split], left, True)
        with jax.named_scope("top_first"):
            top_square.first_hop()
        with jax.named_scope("columns_arrive"):
            old.columns_arrive()

        @pl.when(old.urgent(g, 0))
        def _():
            old.columns_send()

        with jax.named_scope("top_second"):
            top_square.second_hop()
        with jax.named_scope("columns_pass"):
            for dx in range(1, 4):
                @pl.when(old.urgent(g, dx))
                def _():
                    old.pass_column(dx)

        with jax.named_scope("top_third"):
            top_square.third_hop()
        with jax.named_scope("columns_finish"):
            for dx in range(4):
                @pl.when(old.urgent(1 - g, dx))
                def _():
                    old.finish_column(dx)

        @pl.when(jnp.logical_not(old.urgent(g, 0)))
        def _():
            old.columns_send()

        with jax.named_scope("low_first"):
            low_square.first_hop()
        near = cols[lo, :]
        near_scaled = (near.astype(F32) * before).astype(BF16)
        both = times(near_scaled, near, NT) + times(near, near_scaled, NT)
        with jax.named_scope("top_finish"):
            top_square.finish()

        def middle():
            with jax.named_scope("hook0"):
                low_square.second_hop()
                old.pass_rows()

        def late():
            with jax.named_scope("hook1"):
                for dx in range(1, 4):
                    @pl.when(jnp.logical_not(old.urgent(g, dx)))
                    def _():
                        old.pass_column(dx)

        def last():
            with jax.named_scope("hook2"):
                low_square.third_hop()

        with jax.named_scope("factor0"):
            solver, given = factor(
                corner[...] - 0.5 * both, orders[0:1, :], (middle, late, nothing), *scratch
            )
        values[0] = jnp.broadcast_to(given, (128, WIDTH))
        last()
        with jax.named_scope("wait_rows"):
            fetch.wait()
            old.finish_rows()
        with jax.named_scope("panel0"):
            keep_old()
            panel = front[:, lo] - times(rows_scaled[...], near, NT)
            shown = times(panel, solver, NT, EXACT).astype(BF16)
            left[...] = shown
        with jax.named_scope("wait_low"):
            for dx in range(4):
                @pl.when(jnp.logical_not(old.urgent(1 - g, dx)))
                def _():
                    old.finish_column(dx)

            low_square.finish()
        with jax.named_scope("edge"):
            next_near = cols[hi, :]
            next_scaled = (next_near.astype(F32) * before).astype(BF16)
            edge = edges[:, lo] - times(next_scaled, near, NT)
            edge = times(edge, solver, NT, EXACT).astype(BF16)
        with jax.named_scope("scatter"):
            for to in range(1, 16):
                handed(0, 0, to).start()
            new.begin()
            for to in range(1, 16):
                handed(1, 0, to).start()
        edge_scaled = (edge.astype(F32) * given).astype(BF16)
        both = times(next_scaled, next_near, NT) + times(next_near, next_scaled, NT)
        more = times(edge_scaled, edge, NT) + times(edge, edge_scaled, NT)
        square = (edges[:, hi] - 0.5 * both) - 0.5 * more

        with jax.named_scope("factor1"):
            solver, later = factor(
                square, orders[1:2, :], (nothing, nothing, nothing), *scratch
            )
        values[1] = jnp.broadcast_to(later, (128, WIDTH))
        with jax.named_scope("panel1"):
            shown_scaled = (left[...].astype(F32) * given).astype(BF16)
            panel = front[:, hi] - times(rows_scaled[...], next_near, NT)
            panel = panel - times(shown_scaled, edge, NT)
            right[...] = times(panel, solver, NT, EXACT).astype(BF16)
        @pl.when(q != 0)
        def _():
            new_left[...] = shown_scaled

        @pl.when(q == 0)
        def _():
            new_left[lo, :] = jnp.zeros_like(new_left[lo, :])
            new_left[hi, :] = shown_scaled[hi]

        chunk[...] = left[0:CHUNK, :]
        shared[...] = values[:, 0:8, :]
        for to in range(1, 16):
            handed(1, 1, to).start()
            handed(0, 1, to).start()
        second[...] = right[0:CHUNK, :]
        with jax.named_scope("arrive"):
            new.columns_arrive()

        @pl.when(g == 1)
        def _():
            new.columns_send()

        with jax.named_scope("apply_old"):
            apply_old()
        new_cols[lo, :] = jnp.zeros((WIDTH, WIDTH), BF16)
        new_cols[hi, :] = edge
        keep_near.start()
        keep_left.start()
        with jax.named_scope("last_columns"):
            @pl.when(g == 1)
            def _():
                new.pass_columns()

            @pl.when(g == 0)
            def _():
                new.finish_columns()

        keep_far.start()

    @pl.when(c != 0)
    def _():
        with jax.named_scope("old"):
            old.pass_rows()
            old.columns_arrive()
            old.columns_send()
            old.pass_columns()
            old.finish_rows()
            old.finish_columns()
        keep_old()
        fetch.wait()
        apply_old()
        new = Spread(chunk, new_rows, new_cols, sems[split:2 * split], None, True)
        with jax.named_scope("recv_chunk"):
            handed(0, 0, c).wait_recv()
        new.begin()
        with jax.named_scope("pass_rows"):
            new.pass_rows()
        with jax.named_scope("columns_arrive"):
            new.columns_arrive()
            new.columns_send()
        with jax.named_scope("pass_columns"):
            new.pass_columns()
        with jax.named_scope("finish_rows"):
            new.finish_rows()
            handed(1, 0, c).wait_recv()
        given = shared[0, 0:1, :]

        @pl.when(q != 0)
        def _():
            new_left[...] = (new_rows[...].astype(F32) * given).astype(BF16)

        @pl.when(q == 0)
        def _():
            new_left[lo, :] = jnp.zeros_like(new_left[lo, :])
            new_left[hi, :] = (new_rows[hi, :].astype(F32) * given).astype(BF16)

        keep_left.start()
        with jax.named_scope("finish_columns"):
            new.finish_columns()
        keep_right.start()
        with jax.named_scope("recv_values"):
            handed(1, 1, c).wait_recv()
            handed(0, 1, c).wait_recv()
        new.drain()
        new.drain_columns()

    given, later = shared[0, 0:1, :], shared[1, 0:1, :]
    panels[:, lo] = chunk[...].astype(F32) * given
    live = (q != 0) | (c >= WIDTH // CHUNK)

    @pl.when(live)
    def _():
        panels[:, hi] = second[...].astype(F32) * later

    @pl.when(jnp.logical_not(live))
    def _():
        panels[:, hi] = jnp.zeros((CHUNK, WIDTH), F32)

    pivots_kept[:, lo] = given
    pivots_kept[:, hi] = later
    keep_panels.start()
    keep_pivots.start()
    @pl.when(c == 0)
    def _():
        new = Spread(block(left, 0, CHUNK), new_rows, new_cols, sems[split:2 * split], left, True)
        with jax.named_scope("drain_last"):
            new.own_row_copy().wait()
            new.drain()

            @pl.when(g == 1)
            def _():
                new.drain_columns()

            for panel in range(2):
                rest = (left, right)[panel].at[CHUNK:16 * CHUNK]
                remote(rest, rest, send.at[panel], recv.at[panel], (1 - g, r, c)).wait_send()
                rest = values.at[panel, 8:128]
                remote(rest, rest, send.at[2 + panel], recv.at[2 + panel], (1 - g, r, c)).wait_send()
            top_square.drain()
            low_square.drain()
            keep_near.wait()
            keep_far.wait()

    @pl.when(c != 0)
    def _():
        keep_right.wait()

    with jax.named_scope("drain_old"):
        old.drain()
        old.drain_columns()
        for copy in (*keeping, keep_left, keep_panels, keep_pivots):
            copy.wait()


def apply_kernel(front, new_left, new_right, panels, pivots,
                 schur, panels_out, pivots_out,
                 tiles, results, left, right, front_in, left_in, right_in, out,
                 panels_kept, pivots_kept, small_in, small_out):
    wide = front.shape[1] // TILES
    side = pltpu.make_async_copy(new_left, left, left_in)
    side.start()
    fetches = []
    for j in range(TILES):
        at = pl.ds(j * wide, wide)
        group = (
            pltpu.make_async_copy(new_right.at[at], right.at[at], right_in.at[j]),
            pltpu.make_async_copy(front.at[:, at], tiles.at[j], front_in.at[j]),
        )
        for copy in group:
            copy.start()
        fetches.append(group)
    small = (
        (panels, panels_kept, panels_out),
        (pivots, pivots_kept, pivots_out),
    )
    arrivals = [
        pltpu.make_async_copy(a, b, small_in.at[n]) for n, (a, b, _) in enumerate(small)
    ]
    leaving = [
        pltpu.make_async_copy(b, c, small_out.at[n]) for n, (_, b, c) in enumerate(small)
    ]
    for copy in arrivals:
        copy.start()
    side.wait()
    stores = []
    for j in range(TILES):
        for copy in fetches[j]:
            copy.wait()
        rows = slice(j * wide, (j + 1) * wide)
        results[j] = tiles[j] - times(left[...], right[rows, :], NT)
        store = pltpu.make_async_copy(
            results.at[j], schur.at[:, pl.ds(j * wide, wide)], out.at[j]
        )
        store.start()
        stores.append(store)
        if j == 0:
            for copy, onward in zip(arrivals, leaving):
                copy.wait()
                onward.start()
    for store in stores + leaving:
        store.wait()


def body(front, prev_lower, prev_pivots, pivot_order):
    row_count, col_count = front.shape
    width = prev_lower.shape[1]
    vmem = pl.BlockSpec(memory_space=pltpu.VMEM)
    anywhere = pl.BlockSpec(memory_space=pl.ANY)
    shape = jax.ShapeDtypeStruct
    dma = pltpu.SemaphoreType.DMA
    scratch = pltpu.VMEM
    updated, new_left, new_right, panels, pivots = pl.pallas_call(
        window_kernel,
        out_shape=[
            shape((row_count, col_count), F32),
            shape((row_count, width), BF16),
            shape((col_count, width), BF16),
            shape((CHUNK, 2 * width), F32),
            shape((1, 2 * width), F32),
        ],
        in_specs=[anywhere] * 4,
        out_specs=[anywhere] * 5,
        scratch_shapes=[
            scratch((CHUNK, width), BF16),
            scratch((1, width), F32),
            scratch(pivot_order.shape, jnp.int32),
            scratch((CHUNK, 2 * width), F32),
            scratch((1, 2 * width), F32),
            dma((3,)),
            scratch((row_count, width), BF16),
            scratch((row_count, width), BF16),
            scratch((col_count, width), BF16),
            scratch((row_count, width), BF16),
            scratch((row_count, width), BF16),
            scratch((col_count, width), BF16),
            scratch((CHUNK, width), BF16),
            scratch((CHUNK, width), BF16),
            scratch((2, 8, width), F32),
            scratch((row_count, width), BF16),
            scratch((row_count, width), BF16),
            scratch((2, 128, width), F32),
            scratch((width, width), F32),
            scratch((width, 2 * width), F32),
            scratch((row_count, col_count), F32),
            dma,
            dma((TILES,)),
            dma((6,)),
            scratch((HALF, 2 * HALF), F32),
            scratch((2 * HALF, HALF), F32),
            scratch((2 * HALF, HALF), F32),
            scratch((2 * HALF, HALF), F32),
            scratch((8 * HALF, HALF), F32),
            scratch((HALF, HALF), F32),
            dma((4,)),
            dma((4,)),
        ]
        + Spread.semaphores() * 2
        + Corner.semaphores() * 2,
        compiler_params=pltpu.CompilerParams(
            collective_id=0, has_side_effects=True, vmem_limit_bytes=VMEM_LIMIT
        ),
        name="window",
    )(prev_lower, front, prev_pivots.reshape(1, width), pivot_order)
    tile = col_count // TILES
    schur, panels, pivots = pl.pallas_call(
        apply_kernel,
        out_shape=[
            shape((row_count, col_count), F32),
            shape((CHUNK, 2 * width), F32),
            shape((1, 2 * width), F32),
        ],
        in_specs=[anywhere] * 5,
        out_specs=[anywhere] * 3,
        scratch_shapes=[
            scratch((TILES, row_count, tile), F32),
            scratch((TILES, row_count, tile), F32),
            scratch((row_count, width), BF16),
            scratch((col_count, width), BF16),
            dma((TILES,)),
            dma,
            dma((TILES,)),
            dma((TILES,)),
            scratch((CHUNK, 2 * width), F32),
            scratch((1, 2 * width), F32),
            dma((2,)),
            dma((2,)),
        ],
        compiler_params=pltpu.CompilerParams(vmem_limit_bytes=VMEM_LIMIT),
        name="apply",
    )(updated, new_left, new_right, panels, pivots)
    return schur, panels, pivots.reshape(2 * width)


def solution(mesh):
    in_specs = (P(("grp", "row"), "col"), P(("grp", "row", "col"), None), P(), P())
    out_specs = (P(("grp", "row"), "col"), P(("grp", "row", "col"), None), P())
    return jax.shard_map(body, mesh=mesh, in_specs=in_specs, out_specs=out_specs, check_vma=False)
```
